256 devices in a mesh: tm: 32 (over y, z_lo, core), space: 8 (over z_hi, x).
Axes of the slice: x: 4, y: 4, z: 8 (z_hi: 2, z_lo: 4; z = z_hi * 4 + z_lo), core: 2. Of those that a mesh axis runs over, the one named last changes fastest.
Arguments:
- forcing: float32 [64, 128, 128, 128], P('tm', 'space'), may hold values from -24 to 24
- exponents: int32 [64], P('tm'), may hold values from 0 to 8
- mixing: float32 [64, 64], replicated, may hold values from -1 to 3, as said below
- unmixing: float32 [64, 64], replicated, may hold values from -1 to 1
Outputs:
- solution: float32 [64, 128, 128, 128], P('tm', 'space')
The draws below stay inside these ranges and needn't reach their ends.
Inputs may be any that keep to these rules, and one draw needn't show every extreme that they name: unmixing is the inverse of mixing up to float32 rounding.
All inputs are finite; a program needn't handle non-finite values.
Results may differ from the reference program's by a relative error of at most 0.00027.
Values sent between devices are 32-bit elements; how exact they have to be, the bound alone decides.
A program may use at most 64 MiB of HBM per device.

```python
import math
import jax
import jax.numpy as jnp
from jax import lax

N = 128
STEPS = 64


def shared_pair(key):
    order = STEPS
    folded = jax.random.fold_in(key, 4711)
    diagonal_key, offdiag_key = jax.random.split(folded)
    diagonal = jax.random.uniform(diagonal_key, (order,), jnp.float32, 1.2, 2.0)
    offdiag = jnp.clip(jax.random.normal(offdiag_key, (order, order), jnp.float32), -4.0, 4.0)
    matrix = jnp.diag(diagonal) + 0.4 / math.sqrt(order) * offdiag
    inverse = jnp.linalg.solve(matrix, jnp.eye(order, dtype=jnp.float32))
    return (matrix, inverse)


def draw_mixing(key, part):
    return shared_pair(key)[0]


def draw_unmixing(key, part):
    return shared_pair(key)[1]


def draw_forcing(key, part):
    folded = jax.random.fold_in(key, 913)
    rough_key, amp_key = jax.random.split(folded)
    return jnp.clip(4.0 * jax.random.normal(rough_key, (STEPS, N, N, N), jnp.float32), -24.0, 24.0)


def plant(entries, rng, least, largest):
    extent = entries.shape
    place = [jax.random.randint(jax.random.fold_in(rng, axis), (), 0, extent[axis]) for axis in range(len(extent))]
    entries = entries.at[tuple(place)].set(least)
    longest = extent.index(max(extent))
    place[longest] = (place[longest] + 1) % extent[longest]
    return entries.at[tuple(place)].set(largest)


def setup_inputs(seed: int = 0) -> dict:
    streams_of = jax.random.split(jax.random.key(seed), 5)
    forcing = draw_forcing(jax.random.fold_in(streams_of[4], 71), 0)
    exponents = plant(jax.random.randint(streams_of[1], (STEPS,), 0, 9), jax.random.fold_in(streams_of[1], 1), 0, 8).astype(jnp.int32)
    mixing = draw_mixing(jax.random.fold_in(streams_of[4], 71), 0)
    unmixing = draw_unmixing(jax.random.fold_in(streams_of[4], 71), 0)
    return dict(forcing=forcing, exponents=exponents, mixing=mixing, unmixing=unmixing)


exact_mode = lax.Precision.HIGHEST

def sine_matrix(length):
    ordinal = jnp.arange(length, dtype=jnp.float32) + 1.0
    angle_step = jnp.pi / (length + 1)
    return jnp.sqrt(2.0 / (length + 1.0)) * jnp.sin(angle_step * ordinal[:, None] * ordinal[None, :])

def eigen_values(length):
    ordinal = jnp.arange(length, dtype=jnp.float32) + 1.0
    return 2.0 - 2.0 * jnp.cos(jnp.pi * ordinal / (length + 1))

def transform(grid_field, matrix):
    grid_field = jnp.einsum('abc,ak->kbc', grid_field, matrix, precision=exact_mode)
    grid_field = jnp.einsum('abc,bk->akc', grid_field, matrix, precision=exact_mode)
    return jnp.dot(grid_field, matrix, precision=exact_mode)

def reference(forcing, exponents, mixing, unmixing):
    step_count = forcing.shape[0]
    length = forcing.shape[1]
    transform_matrix = sine_matrix(length)
    eigen_all = eigen_values(length)
    denom_base = eigen_all[:, None, None] + eigen_all[None, :, None] + eigen_all[None, None, :]
    shifts = 2.0 ** (exponents.astype(jnp.float32) / 4.0)
    unmixed = jnp.dot(unmixing, forcing.reshape(step_count, -1), precision=exact_mode).reshape(forcing.shape)

    def solve_one(packed):
        grid_field, shift_val = packed
        spectral_field = transform(grid_field, transform_matrix)
        return transform(spectral_field / (shift_val + denom_base), transform_matrix)
    solved_field = lax.map(solve_one, (unmixed, shifts))
    return jnp.dot(mixing, solved_field.reshape(step_count, -1), precision=exact_mode).reshape(forcing.shape)
```

```python
import functools

import jax
import jax.numpy as jnp
import numpy as np
from jax import lax
from jax.experimental import pallas as pl
from jax.experimental.pallas import tpu as pltpu
from jax.sharding import PartitionSpec as P

MESH = pl.DeviceIdType.MESH
F32, BF16 = jnp.float32, jnp.bfloat16
N, STEPS = 128, 64
NY, NZ, NC, NH, NX = 4, 4, 2, 2, 4
NT = NY * NZ * NC
LOCAL = N // (NH * NX)
ROWS = LOCAL * NX
HALF = N // 2
SLOTS = NT * NX


def two_parts(x):
    x = np.asarray(x, np.float32)
    high = x.astype(jnp.bfloat16)
    low = (x - high.astype(np.float32)).astype(jnp.bfloat16)
    return high, low


def constants():
    order = np.arange(1, N + 1, dtype=np.float64)
    sine = np.sqrt(2.0 / (N + 1)) * np.sin(np.pi / (N + 1) * order[:, None] * order[None, :])
    mu = 2.0 - 2.0 * np.cos(np.pi * order / (N + 1))
    both = np.zeros((2, N, 2, 2, HALF))
    for step in range(2):
        both[step, :, :, step, :] = sine.reshape(N, 2, HALF)
    both = both.reshape(2 * N, 2 * N)
    into = np.stack(two_parts(both))
    back = np.stack(two_parts(both.T))
    high, low = two_parts(sine)
    stacked = np.concatenate([high, high, low], axis=1)
    tail = np.zeros((8, N))
    for chunk in range(2):
        tail[chunk] = np.tile(mu[chunk * HALF : (chunk + 1) * HALF] + 2.0, 2)
    return into, back, stacked, tail.astype(np.float32), mu.astype(np.float32)


def split(x):
    high = x.astype(BF16)
    low = (x - high.astype(F32)).astype(BF16)
    return high, low


def dot(a, b):
    return jnp.dot(a, b, preferred_element_type=F32)


def packed_mixer(matrix):
    row = lax.broadcasted_iota(jnp.int32, (NT, STEPS), 0)
    col = lax.broadcasted_iota(jnp.int32, (NT, STEPS), 1)
    even = (col == 2 * row).astype(BF16)
    odd = (col == 2 * row + 1).astype(BF16)
    row = lax.broadcasted_iota(jnp.int32, (STEPS, STEPS), 0)
    col = lax.broadcasted_iota(jnp.int32, (STEPS, STEPS), 1)
    pos = 2 * (col - jnp.where(col >= NT, NT, 0))
    upper = jnp.where(col >= NT, 1, 0)
    even_first = (row == pos + upper).astype(BF16)
    odd_first = (row == pos + 1 - upper).astype(BF16)

    def arranged(part):
        top = dot(dot(even, part).astype(BF16), even_first)
        bottom = dot(dot(odd, part).astype(BF16), odd_first)
        return jnp.concatenate([top, bottom], axis=0).astype(BF16)

    high, low = split(matrix)
    high, low = arranged(high), arranged(low)
    return jnp.concatenate([high, high, low], axis=1)


def kernel(
    forcing, exponents, mixing, unmixing, into_c, back_c, sine_c, tail_c, mu,
    out,
    x, into, back, sine, tail, mix_v, unmix_v, mixer, unmixer,
    sent, got, work, ratio, shift, swap_out, swap_in, sent_back, got_back, half_done,
    in_sem, const_sem, send_sem, recv_sem, swap_send, swap_recv, shift_send, shift_recv,
):
    tm, space = lax.axis_index("tm"), lax.axis_index("space")
    y, z, c = tm // (NZ * NC), (tm // NC) % NZ, tm % NC
    h, sx = space // NX, space % NX
    mine = tm * NX + sx
    zs = [(z + d) % NZ for d in range(NZ)]

    def peer(dz, s):
        dx, dy, dc = s % NX, (s // NX) % NY, s // (NX * NY)
        t = ((y + dy) % NY) * (NZ * NC) + zs[dz] * NC + (c + dc) % NC
        px = (sx + dx) % NX
        return t, px

    barrier = pltpu.get_barrier_semaphore()
    for dz in range(NZ):

        @pl.loop(0 if dz else 1, NY * NX * NC)
        def _(s):
            t, px = peer(dz, s)
            pl.semaphore_signal(barrier, inc=1, device_id=(t, h * NX + px), device_id_type=MESH)

    other = (tm, (1 - h) * NX + sx)
    pl.semaphore_signal(barrier, inc=1, device_id=other, device_id_type=MESH)

    loads = [pltpu.make_async_copy(forcing, x, in_sem)]
    pairs = ((into_c, into), (back_c, back), (sine_c, sine), (tail_c, tail), (mixing, mix_v), (unmixing, unmix_v))
    loads += [pltpu.make_async_copy(a, b, const_sem.at[k]) for k, (a, b) in enumerate(pairs)]
    for load in loads:
        load.start()

    lane = lax.broadcasted_iota(jnp.int32, (8, N), 1)
    exponent = jnp.where(lane < HALF, exponents[0].astype(F32), exponents[1].astype(F32))
    my_shift = jnp.exp2(exponent * 0.25)
    shift[tm] = my_shift

    with jax.named_scope("load"):
        loads[0].wait()
        loads[1].wait()
        loads[3].wait()

    with jax.named_scope("first"):

        @pl.loop(0, LOCAL)
        def _(i):
            field = jnp.concatenate([x[0, i], x[1, i]], axis=1)
            high, low = split(field)
            field = dot(high, into[0]) + dot(low, into[0]) + dot(high, into[1])
            high, low = split(field)
            field = dot(sine[...], jnp.concatenate([high, low, high], axis=0))
            sent[0, pl.ds(i, N, stride=LOCAL), :] = field[:, :N]
            sent[1, pl.ds(i, N, stride=LOCAL), :] = field[:, N:]

    with jax.named_scope("barrier"):
        pl.semaphore_wait(barrier, SLOTS)

    def rows(slot):
        return pl.ds(pl.multiple_of(slot * LOCAL, LOCAL), LOCAL)

    def issue(stage, chunk, source, target, groups):
        for dz in groups:

            @pl.loop(0 if dz else 1, NY * NX * NC)
            def _(s):
                t, px = peer(dz, s)
                pltpu.make_async_remote_copy(
                    source.at[chunk, rows(t * NX + px)],
                    target.at[chunk, rows(mine)],
                    send_sem.at[stage, chunk],
                    recv_sem.at[stage, chunk],
                    device_id=(t, h * NX + px),
                    device_id_type=MESH,
                ).start()

    def arrived(stage, chunk, target):
        all_others = target.at[chunk, pl.ds(0, (SLOTS - 1) * LOCAL)]
        pltpu.make_async_copy(all_others, all_others, recv_sem.at[stage, chunk]).wait()

    def left(stage, chunk, source):
        all_others = source.at[chunk, pl.ds(0, (SLOTS - 1) * LOCAL)]
        pltpu.make_async_copy(all_others, all_others, send_sem.at[stage, chunk]).wait()

    def shift_copy(t, k):
        return pltpu.make_async_remote_copy(
            shift.at[tm], shift.at[tm], shift_send, shift_recv, device_id=(t, space), device_id_type=MESH
        )

    for dz in (2, 3, 1, 0):

        @pl.loop(0 if dz else 1, NY * NC)
        def _(s):
            t = ((y + s % NY) % NY) * (NZ * NC) + zs[dz] * NC + (c + s // NY) % NC
            shift_copy(t, s).start()

    with jax.named_scope("issue0"):
        issue(0, 0, sent, got, (2, 3, 1, 0))
        issue(0, 1, sent, got, (2,))
    for chunk in range(2):
        got[chunk, rows(mine), :] = sent[chunk, rows(mine), :]

    loads[4].wait()
    loads[5].wait()
    loads[6].wait()
    mixer[...] = packed_mixer(mix_v[...])
    unmixer[...] = packed_mixer(unmix_v[...])

    pltpu.make_async_copy(shift.at[pl.ds(0, NT - 1)], shift.at[pl.ds(0, NT - 1)], shift_recv).wait()
    shifts = jnp.concatenate([shift[t, 0:1, :] for t in range(NT)], axis=0)
    for chunk in range(2):
        center = shifts + mu[mine] + tail[chunk : chunk + 1, :]

        def step(s, last, chunk=chunk, center=center):
            last = 1.0 / (center - last)
            ratio[chunk, s] = last
            return last

        lax.fori_loop(0, ROWS, step, jnp.zeros((NT, N), F32), unroll=4)

    lower = lax.broadcasted_iota(jnp.int32, (NT, N), 1) < HALF

    def mixed(matrix, field):
        high, low = split(jnp.concatenate([field, pltpu.roll(field, HALF, 1)], axis=0))
        both = dot(matrix, jnp.concatenate([high, low, high], axis=0))
        return jnp.where(lower, both[:NT], both[NT:])

    def place(s):
        return s + h * (ROWS - 1 - 2 * s)

    def swap(chunk):
        return pltpu.make_async_remote_copy(
            swap_out.at[chunk], swap_in.at[chunk], swap_send.at[chunk], swap_recv.at[chunk],
            device_id=other, device_id_type=MESH,
        )

    def towards(chunk):
        with jax.named_scope("wait_got"):
            arrived(0, chunk, got)
        matrix = unmixer[...]

        def unmix(s, _):
            work[chunk, s] = mixed(matrix, got[chunk, pl.ds(place(s), NT, stride=ROWS), :])
            return _

        with jax.named_scope("unmix"):
            lax.fori_loop(0, ROWS, unmix, 0, unroll=4)

        def step(s, last):
            last = (work[chunk, s] + last) * ratio[chunk, s]
            work[chunk, s] = last
            return last

        with jax.named_scope("eliminate"):
            swap_out[chunk] = lax.fori_loop(0, ROWS, step, jnp.zeros((NT, N), F32), unroll=8)
        swap(chunk).start()

    def away(chunk):
        with jax.named_scope("wait_swap"):
            swap(chunk).wait()
        end = ratio[chunk, ROWS - 1]
        edge = (swap_out[chunk] + end * swap_in[chunk]) / (1.0 - end * end)
        work[chunk, ROWS - 1] = edge

        def step(k, last):
            s = ROWS - 2 - k
            last = work[chunk, s] + ratio[chunk, s] * last
            work[chunk, s] = last
            return last

        with jax.named_scope("back"):
            lax.fori_loop(0, ROWS - 1, step, edge, unroll=7)
        matrix = mixer[...]

        def mix(s, _):
            sent_back[chunk, pl.ds(place(s), NT, stride=ROWS), :] = mixed(matrix, work[chunk, s])
            return _

        with jax.named_scope("mix"):
            lax.fori_loop(0, ROWS, mix, 0, unroll=4)
        got_back[chunk, rows(mine), :] = sent_back[chunk, rows(mine), :]

    towards(0)
    issue(0, 1, sent, got, (3, 1, 0))
    away(0)
    issue(1, 0, sent_back, got_back, (2, 3))
    towards(1)
    issue(1, 0, sent_back, got_back, (1, 0))
    away(1)
    issue(1, 1, sent_back, got_back, (2, 3, 1, 0))

    def second(chunk, i):
        high, low = split(got_back[chunk, pl.ds(i, N, stride=LOCAL), :])
        return dot(sine[...], jnp.concatenate([high, low, high], axis=0))

    loads[2].wait()
    with jax.named_scope("wait_back0"):
        arrived(1, 0, got_back)

    with jax.named_scope("last0"):

        @pl.loop(0, LOCAL)
        def _(i):
            half_done[i] = second(0, i)

    with jax.named_scope("wait_back1"):
        arrived(1, 1, got_back)

    with jax.named_scope("last1"):

        @pl.loop(0, LOCAL)
        def _(i):
            high, low = split(jnp.concatenate([half_done[i], second(1, i)], axis=1))
            field = dot(high, back[0]) + dot(low, back[0]) + dot(high, back[1])
            out[0, i] = field[:, :N]
            out[1, i] = field[:, N:]

    for chunk in range(2):
        left(0, chunk, sent)
        left(1, chunk, sent_back)
    pltpu.make_async_copy(shift.at[pl.ds(0, NT - 1)], shift.at[pl.ds(0, NT - 1)], shift_send).wait()


def body(forcing, exponents, mixing, unmixing):
    into, back, stacked, tail, mu = constants()
    whole = pl.BlockSpec(memory_space=pltpu.HBM)
    smem = pl.BlockSpec(memory_space=pltpu.SMEM)
    dma = pltpu.SemaphoreType.DMA
    packed = (2, SLOTS * LOCAL, N)
    return pl.pallas_call(
        kernel,
        out_shape=jax.ShapeDtypeStruct(forcing.shape, F32),
        in_specs=[whole, smem, whole, whole, whole, whole, whole, whole, smem],
        out_specs=pl.BlockSpec(memory_space=pltpu.VMEM),
        scratch_shapes=[
            pltpu.VMEM(forcing.shape, F32),
            pltpu.VMEM(into.shape, BF16),
            pltpu.VMEM(back.shape, BF16),
            pltpu.VMEM(stacked.shape, BF16),
            pltpu.VMEM(tail.shape, F32),
            pltpu.VMEM((STEPS, STEPS), F32),
            pltpu.VMEM((STEPS, STEPS), F32),
            pltpu.VMEM((STEPS, 3 * STEPS), BF16),
            pltpu.VMEM((STEPS, 3 * STEPS), BF16),
            pltpu.VMEM(packed, F32),
            pltpu.VMEM(packed, F32),
            pltpu.VMEM((2, ROWS, NT, N), F32),
            pltpu.VMEM((2, ROWS, NT, N), F32),
            pltpu.VMEM((NT, 8, N), F32),
            pltpu.VMEM((2, NT, N), F32),
            pltpu.VMEM((2, NT, N), F32),
            pltpu.VMEM(packed, F32),
            pltpu.VMEM(packed, F32),
            pltpu.VMEM((LOCAL, N, N), F32),
            dma,
            dma((6,)),
            dma((2, 2)),
            dma((2, 2)),
            dma((2,)),
            dma((2,)),
            dma,
            dma,
        ],
        compiler_params=pltpu.CompilerParams(
            collective_id=0, has_side_effects=True, vmem_limit_bytes=60 * 1024 * 1024
        ),
        name="heat",
    )(forcing, exponents, mixing, unmixing, into, back, stacked, tail, mu)


def solution(mesh):
    placed = (P("tm", "space", None, None), P("tm"), P(), P())
    return jax.shard_map(
        body, mesh=mesh, in_specs=placed, out_specs=P("tm", "space", None, None), check_vma=False
    )
```

```python
import functools

import jax
import jax.numpy as jnp
import numpy as np
from jax import lax
from jax.experimental import pallas as pl
from jax.experimental.pallas import tpu as pltpu
from jax.sharding import PartitionSpec as P

MESH = pl.DeviceIdType.MESH
F32, BF16 = jnp.float32, jnp.bfloat16
N, STEPS = 128, 64
NY, NZ, NC, NH, NX = 4, 4, 2, 2, 4
NT = NY * NZ * NC
LOCAL = N // (NH * NX)
ROWS = LOCAL * NX
HALF = N // 2
SLOTS = NT * NX


def two_parts(x):
    x = np.asarray(x, np.float32)
    high = x.astype(jnp.bfloat16)
    low = (x - high.astype(np.float32)).astype(jnp.bfloat16)
    return high, low


def constants():
    order = np.arange(1, N + 1, dtype=np.float64)
    sine = np.sqrt(2.0 / (N + 1)) * np.sin(np.pi / (N + 1) * order[:, None] * order[None, :])
    mu = 2.0 - 2.0 * np.cos(np.pi * order / (N + 1))
    both = np.zeros((2, N, 2, 2, HALF))
    for step in range(2):
        both[step, :, :, step, :] = sine.reshape(N, 2, HALF)
    both = both.reshape(2 * N, 2 * N)
    high, low = two_parts(both)
    into = np.concatenate([high, high, low], axis=0)
    high, low = two_parts(both.T)
    back = np.concatenate([high, high, low], axis=0)
    high, low = two_parts(sine)
    stacked = np.concatenate([high, high, low], axis=1)
    tail = np.zeros((8, N))
    for chunk in range(2):
        tail[chunk] = np.tile(mu[chunk * HALF : (chunk + 1) * HALF] + 2.0, 2)
    return into, back, stacked, tail.astype(np.float32), mu.astype(np.float32)


def split(x):
    high = x.astype(BF16)
    low = (x - high.astype(F32)).astype(BF16)
    return high, low


def dot(a, b):
    return jnp.dot(a, b, preferred_element_type=F32)


def packed_mixer(matrix):
    row = lax.broadcasted_iota(jnp.int32, (NT, STEPS), 0)
    col = lax.broadcasted_iota(jnp.int32, (NT, STEPS), 1)
    even = (col == 2 * row).astype(BF16)
    odd = (col == 2 * row + 1).astype(BF16)
    row = lax.broadcasted_iota(jnp.int32, (STEPS, STEPS), 0)
    col = lax.broadcasted_iota(jnp.int32, (STEPS, STEPS), 1)
    pos = 2 * (col - jnp.where(col >= NT, NT, 0))
    upper = jnp.where(col >= NT, 1, 0)
    even_first = (row == pos + upper).astype(BF16)
    odd_first = (row == pos + 1 - upper).astype(BF16)

    def arranged(part):
        top = dot(dot(even, part).astype(BF16), even_first)
        bottom = dot(dot(odd, part).astype(BF16), odd_first)
        return jnp.concatenate([top, bottom], axis=0).astype(BF16)

    high, low = split(matrix)
    high, low = arranged(high), arranged(low)
    return jnp.concatenate([high, high, low], axis=1)


def kernel(
    forcing, exponents_c, mixing, unmixing, into_c, back_c, sine_c, tail_c, mu_c,
    out,
    exponents, mu, x, first_rows, into, back, sine, tail, mix_v, unmix_v, mixer, unmixer,
    sent, got, work, ratio, shift, swap_out, swap_in, sent_back, got_back, last_rows,
    in_sem, const_sem, send_sem, recv_sem, swap_send, swap_recv, shift_send, shift_recv,
):
    tm, space = lax.axis_index("tm"), lax.axis_index("space")
    y, z, c = tm // (NZ * NC), (tm // NC) % NZ, tm % NC
    h, sx = space // NX, space % NX
    mine = tm * NX + sx
    zs = [(z + d) % NZ for d in range(NZ)]
    xs = [(sx + d) % NX for d in range(NX)]

    quarter = LOCAL // 4
    fields = [
        pltpu.make_async_copy(
            forcing.at[:, pl.ds(b * quarter, quarter)], x.at[:, pl.ds(b * quarter, quarter)], in_sem.at[b]
        )
        for b in range(4)
    ]
    pairs = (
        (into_c, into), (sine_c, sine), (exponents_c, exponents), (mu_c, mu), (tail_c, tail),
        (mixing, mix_v), (unmixing, unmix_v), (back_c, back),
    )
    loads = [pltpu.make_async_copy(a, b, const_sem.at[k]) for k, (a, b) in enumerate(pairs)]
    for load in (loads[0], *fields, *loads[1:]):
        load.start()

    barrier = pltpu.get_barrier_semaphore()
    other = (tm, (1 - h) * NX + sx)

    def greet(i):
        dy, dc = 2 * (i % 2), (i // 2) % 2
        tc = zs[i // 4] * NC + (c + dc) % NC
        for u in range(8):
            t = ((y + dy + u // NX) % NY) * (NZ * NC) + tc
            pl.semaphore_signal(barrier, inc=1, device_id=(t, h * NX + xs[u % NX]), device_id_type=MESH)

    pl.semaphore_signal(barrier, inc=1, device_id=other, device_id_type=MESH)

    with jax.named_scope("greet"):
        for b in range(16):
            greet(b)

    with jax.named_scope("load"):
        loads[0].wait()
        fields[0].wait()

    def into_columns(i):
        high, low = split(jnp.concatenate([x[0, i], x[1, i]], axis=1))
        field = dot(jnp.concatenate([high, low, high], axis=1), into[...])
        high, low = split(field)
        first_rows[0, i] = high
        first_rows[1, i] = low

    def into_rows(i):
        high, low = first_rows[0, i], first_rows[1, i]
        field = dot(sine[...], jnp.concatenate([high, low, high], axis=0))
        sent[0, pl.ds(i, N, stride=LOCAL), :] = field[:, :N]
        sent[1, pl.ds(i, N, stride=LOCAL), :] = field[:, N:]

    with jax.named_scope("first"):
        for i in range(LOCAL):
            if i and i % quarter == 0:
                fields[i // quarter].wait()
            into_columns(i)
    with jax.named_scope("firstb"):
        loads[1].wait()
        for i in range(LOCAL):
            into_rows(i)

    loads[2].wait()
    loads[3].wait()
    lane = lax.broadcasted_iota(jnp.int32, (8, N), 1)
    exponent = jnp.where(lane < HALF, exponents[0].astype(F32), exponents[1].astype(F32))
    shift[tm] = jnp.exp2(exponent * 0.25)

    with jax.named_scope("barrier"):
        pl.semaphore_wait(barrier, SLOTS + 1)

    def rows(slot):
        return pl.ds(pl.multiple_of(slot * LOCAL, LOCAL), LOCAL)

    def issue(stage, chunk, source, target, groups):
        def start(t, px):
            pltpu.make_async_remote_copy(
                source.at[chunk, rows(t * NX + px)],
                target.at[chunk, rows(mine)],
                send_sem.at[stage, chunk],
                recv_sem.at[stage, chunk],
                device_id=(t, h * NX + px),
                device_id_type=MESH,
            ).start()

        for dz in groups:
            for dc in range(NC):
                tc = zs[dz] * NC + (c + dc) % NC

                @pl.loop(0 if dz or dc else 1, NY)
                def _(dy, tc=tc):
                    t = ((y + dy) % NY) * (NZ * NC) + tc
                    for dx in range(NX):
                        start(t, xs[dx])

                if not (dz or dc):
                    for dx in range(1, NX):
                        start(tm, xs[dx])

    def arrived(stage, chunk, target):
        all_others = target.at[chunk, pl.ds(0, (SLOTS - 1) * LOCAL)]
        pltpu.make_async_copy(all_others, all_others, recv_sem.at[stage, chunk]).wait()

    def left(stage, chunk, source):
        all_others = source.at[chunk, pl.ds(0, (SLOTS - 1) * LOCAL)]
        pltpu.make_async_copy(all_others, all_others, send_sem.at[stage, chunk]).wait()

    def shift_copy(t):
        return pltpu.make_async_remote_copy(
            shift.at[tm], shift.at[tm], shift_send, shift_recv, device_id=(t, space), device_id_type=MESH
        )

    with jax.named_scope("issue0"):
        for dz in (2, 3, 1, 0):

            @pl.loop(0 if dz else 1, NY * NC)
            def _(s, dz=dz):
                t = ((y + s % NY) % NY) * (NZ * NC) + zs[dz] * NC + (c + s // NY) % NC
                shift_copy(t).start()

        issue(0, 0, sent, got, (2, 3, 1, 0))
        issue(0, 1, sent, got, (2,))

    for chunk in range(2):
        got[chunk, rows(mine), :] = sent[chunk, rows(mine), :]

    loads[4].wait()
    loads[5].wait()
    loads[6].wait()
    loads[7].wait()
    mixer[...] = packed_mixer(mix_v[...])
    unmixer[...] = packed_mixer(unmix_v[...])

    pltpu.make_async_copy(shift.at[pl.ds(0, NT - 1)], shift.at[pl.ds(0, NT - 1)], shift_recv).wait()
    shifts = jnp.concatenate([shift[t, 0:1, :] for t in range(NT)], axis=0)
    for chunk in range(2):
        center = shifts + mu[mine] + tail[chunk : chunk + 1, :]

        def step(s, last, chunk=chunk, center=center):
            last = 1.0 / (center - last)
            ratio[chunk, s] = last
            return last

        lax.fori_loop(0, ROWS, step, jnp.zeros((NT, N), F32), unroll=4)

    lower = lax.broadcasted_iota(jnp.int32, (NT, N), 1) < HALF

    def mixed(matrix, field):
        high, low = split(jnp.concatenate([field, pltpu.roll(field, HALF, 1)], axis=0))
        both = dot(matrix, jnp.concatenate([high, low, high], axis=0))
        return jnp.where(lower, both[:NT], both[NT:])

    def place(s):
        return s + h * (ROWS - 1 - 2 * s)

    def swap(chunk):
        return pltpu.make_async_remote_copy(
            swap_out.at[chunk], swap_in.at[chunk], swap_send.at[chunk], swap_recv.at[chunk],
            device_id=other, device_id_type=MESH,
        )

    def towards(chunk):
        with jax.named_scope("wait_got"):
            arrived(0, chunk, got)
        matrix = unmixer[...]

        def unmix(s, _):
            work[chunk, s] = mixed(matrix, got[chunk, pl.ds(place(s), NT, stride=ROWS), :])
            return _

        with jax.named_scope("unmix"):
            lax.fori_loop(0, ROWS, unmix, 0, unroll=8)

        def step(s, last):
            last = (work[chunk, s] + last) * ratio[chunk, s]
            work[chunk, s] = last
            return last

        with jax.named_scope("eliminate"):
            swap_out[chunk] = lax.fori_loop(0, ROWS, step, jnp.zeros((NT, N), F32), unroll=8)
        swap(chunk).start()

    def away(chunk):
        with jax.named_scope("wait_swap"):
            swap(chunk).wait()
        end = ratio[chunk, ROWS - 1]
        edge = (swap_out[chunk] + end * swap_in[chunk]) / (1.0 - end * end)
        work[chunk, ROWS - 1] = edge

        def step(k, last):
            s = ROWS - 2 - k
            last = work[chunk, s] + ratio[chunk, s] * last
            work[chunk, s] = last
            return last

        with jax.named_scope("back"):
            lax.fori_loop(0, ROWS - 1, step, edge, unroll=7)
        matrix = mixer[...]

        def mix(s, _):
            sent_back[chunk, pl.ds(place(s), NT, stride=ROWS), :] = mixed(matrix, work[chunk, s])
            return _

        with jax.named_scope("mix"):
            lax.fori_loop(0, ROWS, mix, 0, unroll=8)
        got_back[chunk, rows(mine), :] = sent_back[chunk, rows(mine), :]

    towards(0)
    issue(0, 1, sent, got, (3, 1, 0))
    away(0)
    issue(1, 0, sent_back, got_back, (2, 3))
    towards(1)
    issue(1, 0, sent_back, got_back, (1, 0))
    away(1)
    issue(1, 1, sent_back, got_back, (2, 3, 1, 0))

    def from_rows(chunk, i):
        high, low = split(got_back[chunk, pl.ds(i, N, stride=LOCAL), :])
        field = dot(sine[...], jnp.concatenate([high, low, high], axis=0))
        high, low = split(field)
        last_rows[0, i, :, pl.ds(chunk * N, N)] = high
        last_rows[1, i, :, pl.ds(chunk * N, N)] = low

    def from_columns(i):
        high, low = last_rows[0, i], last_rows[1, i]
        field = dot(jnp.concatenate([high, low, high], axis=1), back[...])
        out[0, i] = field[:, :N]
        out[1, i] = field[:, N:]

    for chunk in range(2):
        with jax.named_scope(f"wait_back{chunk}"):
            arrived(1, chunk, got_back)
        with jax.named_scope(f"last{chunk}"):
            for i in range(LOCAL):
                from_rows(chunk, i)
    with jax.named_scope("last_columns"):
        for i in range(LOCAL):
            from_columns(i)

    for chunk in range(2):
        left(0, chunk, sent)
        left(1, chunk, sent_back)
    pltpu.make_async_copy(shift.at[pl.ds(0, NT - 1)], shift.at[pl.ds(0, NT - 1)], shift_send).wait()


def body(forcing, exponents, mixing, unmixing):
    into, back, stacked, tail, mu = constants()
    whole = pl.BlockSpec(memory_space=pltpu.HBM)
    dma = pltpu.SemaphoreType.DMA
    packed = (2, SLOTS * LOCAL, N)
    return pl.pallas_call(
        kernel,
        out_shape=jax.ShapeDtypeStruct(forcing.shape, F32),
        in_specs=[whole] * 9,
        out_specs=pl.BlockSpec(memory_space=pltpu.VMEM),
        scratch_shapes=[
            pltpu.SMEM(exponents.shape, jnp.int32),
            pltpu.SMEM(mu.shape, F32),
            pltpu.VMEM(forcing.shape, F32),
            pltpu.VMEM((2, LOCAL, N, 2 * N), BF16),
            pltpu.VMEM(into.shape, BF16),
            pltpu.VMEM(back.shape, BF16),
            pltpu.VMEM(stacked.shape, BF16),
            pltpu.VMEM(tail.shape, F32),
            pltpu.VMEM((STEPS, STEPS), F32),
            pltpu.VMEM((STEPS, STEPS), F32),
            pltpu.VMEM((STEPS, 3 * STEPS), BF16),
            pltpu.VMEM((STEPS, 3 * STEPS), BF16),
            pltpu.VMEM(packed, F32),
            pltpu.VMEM(packed, F32),
            pltpu.VMEM((2, ROWS, NT, N), F32),
            pltpu.VMEM((2, ROWS, NT, N), F32),
            pltpu.VMEM((NT, 8, N), F32),
            pltpu.VMEM((2, NT, N), F32),
            pltpu.VMEM((2, NT, N), F32),
            pltpu.VMEM(packed, F32),
            pltpu.VMEM(packed, F32),
            pltpu.VMEM((2, LOCAL, N, 2 * N), BF16),
            dma((4,)),
            dma((8,)),
            dma((2, 2)),
            dma((2, 2)),
            dma((2,)),
            dma((2,)),
            dma,
            dma,
        ],
        compiler_params=pltpu.CompilerParams(
            collective_id=0, has_side_effects=True, vmem_limit_bytes=60 * 1024 * 1024
        ),
        name="heat",
    )(forcing, exponents, mixing, unmixing, into, back, stacked, tail, mu)


def solution(mesh):
    placed = (P("tm", "space", None, None), P("tm"), P(), P())
    return jax.shard_map(
        body, mesh=mesh, in_specs=placed, out_specs=P("tm", "space", None, None), check_vma=False
    )
```

```python
import itertools

import jax
import jax.numpy as jnp
import numpy as np
from jax import lax
from jax.experimental import pallas as pl
from jax.experimental.pallas import tpu as pltpu
from jax.sharding import PartitionSpec as P

MESH = pl.DeviceIdType.MESH
F32, BF16 = jnp.float32, jnp.bfloat16
N, STEPS = 128, 64
NY, NZ, NC, NH, NX = 4, 4, 2, 2, 4
NT = NY * NZ * NC
LOCAL = N // (NH * NX)
ROWS = LOCAL * NX
HALF = N // 2
SLOTS = NT * NX
ORDER = (2, 1, 3, 0)
EARLY, LATE = ORDER[:1], ORDER[1:]
EARLY_BACK, LATE_BACK = ORDER[:1], ORDER[1:]


def two_parts(x):
    x = np.asarray(x, np.float32)
    high = x.astype(jnp.bfloat16)
    low = (x - high.astype(np.float32)).astype(jnp.bfloat16)
    return high, low


def constants():
    order = np.arange(1, N + 1, dtype=np.float64)
    sine = np.sqrt(2.0 / (N + 1)) * np.sin(np.pi / (N + 1) * order[:, None] * order[None, :])
    mu = 2.0 - 2.0 * np.cos(np.pi * order / (N + 1))
    both = np.zeros((2, N, 2, 2, HALF))
    for step in range(2):
        both[step, :, :, step, :] = sine.reshape(N, 2, HALF)
    both = both.reshape(2 * N, 2 * N)
    high, low = two_parts(both)
    into = np.concatenate([high, high, low], axis=0)
    high, low = two_parts(both.T)
    back = np.concatenate([high, high, low], axis=0)
    high, low = two_parts(sine)
    stacked = np.concatenate([high, high, low], axis=1)
    tail = np.zeros((8, N))
    for chunk in range(2):
        tail[chunk] = np.tile(mu[chunk * HALF : (chunk + 1) * HALF] + 2.0, 2)
    return into, back, stacked, tail.astype(np.float32), mu.astype(np.float32)


def split(x):
    high = x.astype(BF16)
    low = (x - high.astype(F32)).astype(BF16)
    return high, low


def dot(a, b):
    return jnp.dot(a, b, preferred_element_type=F32)


def packed_mixer(matrix):
    row = lax.broadcasted_iota(jnp.int32, (NT, STEPS), 0)
    col = lax.broadcasted_iota(jnp.int32, (NT, STEPS), 1)
    even = (col == 2 * row).astype(BF16)
    odd = (col == 2 * row + 1).astype(BF16)
    row = lax.broadcasted_iota(jnp.int32, (STEPS, STEPS), 0)
    col = lax.broadcasted_iota(jnp.int32, (STEPS, STEPS), 1)
    pos = 2 * (col - jnp.where(col >= NT, NT, 0))
    upper = jnp.where(col >= NT, 1, 0)
    even_first = (row == pos + upper).astype(BF16)
    odd_first = (row == pos + 1 - upper).astype(BF16)

    def arranged(part):
        top = dot(dot(even, part).astype(BF16), even_first)
        bottom = dot(dot(odd, part).astype(BF16), odd_first)
        return jnp.concatenate([top, bottom], axis=0).astype(BF16)

    high, low = split(matrix)
    high, low = arranged(high), arranged(low)
    return jnp.concatenate([high, high, low], axis=1)


def kernel(
    forcing, exponents_c, mixing, unmixing, into_c, back_c, sine_c, tail_c, mu_c,
    out,
    exponents, mu, x, first_rows, into, back, sine, tail, mix_v, unmix_v, mixer, unmixer,
    sent, got, work, ratio, shift, swap_out, swap_in, sent_back, got_back, last_rows,
    in_sem, const_sem, send_sem, recv_sem, swap_send, swap_recv, shift_send, shift_recv,
):
    tm, space = lax.axis_index("tm"), lax.axis_index("space")
    y, z, c = tm // (NZ * NC), (tm // NC) % NZ, tm % NC
    h, sx = space // NX, space % NX
    mine = tm * NX + sx
    zs = [z, z + 1 - 2 * (z % 2), (z + 2) % NZ, NZ - 1 - z]
    xs = [(sx + d) % NX for d in range(NX)]
    ys = [(y + d) % NY for d in range(NY)]
    cs = [(c + d) % NC for d in range(NC)]

    quarter = LOCAL // 4
    fields = [
        pltpu.make_async_copy(
            forcing.at[:, pl.ds(b * quarter, quarter)], x.at[:, pl.ds(b * quarter, quarter)], in_sem.at[b]
        )
        for b in range(4)
    ]
    pairs = (
        (into_c, into), (sine_c, sine), (exponents_c, exponents), (mu_c, mu), (tail_c, tail),
        (mixing, mix_v), (unmixing, unmix_v), (back_c, back),
    )
    loads = [pltpu.make_async_copy(a, b, const_sem.at[k]) for k, (a, b) in enumerate(pairs)]
    for load in (loads[0], *fields, *loads[1:]):
        load.start()

    barrier = pltpu.get_barrier_semaphore()
    other = (tm, (1 - h) * NX + sx)

    pl.semaphore_signal(barrier, inc=1, device_id=other, device_id_type=MESH)

    with jax.named_scope("greet"):
        steps = itertools.product(range(NX), range(NY), range(NZ), range(NC))
        farthest_first = sorted(steps, key=lambda d: -min(d[0], NX - d[0]) - min(d[1], NY - d[1]) - 2 * (d[2] > 0))
        for dx, dy, dz, dc in farthest_first[:-2] + [(0, 0, 0, 1)]:
            t = ys[dy] * (NZ * NC) + zs[dz] * NC + cs[dc]
            pl.semaphore_signal(barrier, inc=1, device_id=(t, h * NX + xs[dx]), device_id_type=MESH)

    with jax.named_scope("load"):
        loads[0].wait()
        fields[0].wait()

    def into_columns(i):
        high, low = split(jnp.concatenate([x[0, i], x[1, i]], axis=1))
        field = dot(jnp.concatenate([high, low, high], axis=1), into[...])
        high, low = split(field)
        first_rows[0, i] = high
        first_rows[1, i] = low

    def into_rows(chunk, i):
        columns = pl.ds(chunk * N, N)
        high, low = (
            jnp.concatenate([first_rows[k, i, :, columns], first_rows[k, i + 1, :, columns]], axis=1) for k in range(2)
        )
        field = dot(sine[...], jnp.concatenate([high, low, high], axis=0))
        sent[chunk, pl.ds(i, N, stride=LOCAL), :] = field[:, :N]
        sent[chunk, pl.ds(i + 1, N, stride=LOCAL), :] = field[:, N:]

    def rows(slot, part=0, parts=1):
        length = LOCAL // parts
        return pl.ds(pl.multiple_of(slot * LOCAL + part * length, length), length)

    def issue(stage, chunk, source, target, groups, *part):
        def start(t, px):
            pltpu.make_async_remote_copy(
                source.at[chunk, rows(t * NX + px, *part)],
                target.at[chunk, rows(mine, *part)],
                send_sem.at[stage, chunk],
                recv_sem.at[stage, chunk],
                device_id=(t, h * NX + px),
                device_id_type=MESH,
            ).start()

        for dz in groups:
            for dc in range(NC):
                tc = zs[dz] * NC + (c + dc) % NC

                @pl.loop(0 if dz or dc else 1, NY)
                def _(dy, tc=tc):
                    t = ((y + dy) % NY) * (NZ * NC) + tc
                    for dx in range(NX):
                        start(t, xs[dx])

                if not (dz or dc):
                    for dx in range(1, NX):
                        start(tm, xs[dx])

    loads[2].wait()
    loads[3].wait()
    lane = lax.broadcasted_iota(jnp.int32, (8, N), 1)
    exponent = jnp.where(lane < HALF, exponents[0].astype(F32), exponents[1].astype(F32))
    shift[tm] = jnp.exp2(exponent * 0.25)

    def shift_copy(t):
        return pltpu.make_async_remote_copy(
            shift.at[tm], shift.at[tm], shift_send, shift_recv, device_id=(t, space), device_id_type=MESH
        )

    def issue_shifts():
        for dz in ORDER:

            @pl.loop(0 if dz else 1, NY * NC)
            def _(s, dz=dz):
                t = ((y + s % NY) % NY) * (NZ * NC) + zs[dz] * NC + (c + s // NY) % NC
                shift_copy(t).start()

    for half in range(2):
        with jax.named_scope(f"first{half}"):
            for i in range(half * LOCAL // 2, (half + 1) * LOCAL // 2):
                if i and i % quarter == 0:
                    fields[i // quarter].wait()
                into_columns(i)
            if not half:
                loads[1].wait()
            for i in range(half * LOCAL // 2, (half + 1) * LOCAL // 2, 2):
                into_rows(0, i)
        if not half:
            with jax.named_scope("barrier"):
                pl.semaphore_wait(barrier, SLOTS)
            issue_shifts()
        issue(0, 0, sent, got, ORDER[:1], half, 2)

    def arrived(stage, chunk, target):
        all_others = target.at[chunk, pl.ds(0, (SLOTS - 1) * LOCAL)]
        pltpu.make_async_copy(all_others, all_others, recv_sem.at[stage, chunk]).wait()

    def left(stage, chunk, source):
        all_others = source.at[chunk, pl.ds(0, (SLOTS - 1) * LOCAL)]
        pltpu.make_async_copy(all_others, all_others, send_sem.at[stage, chunk]).wait()

    with jax.named_scope("issue0"):
        issue(0, 0, sent, got, ORDER[1:])
    with jax.named_scope("first2"):
        for i in range(0, LOCAL, 2):
            into_rows(1, i)
    issue(0, 1, sent, got, EARLY)
    for chunk in range(2):
        got[chunk, rows(mine), :] = sent[chunk, rows(mine), :]

    loads[4].wait()
    loads[5].wait()
    loads[6].wait()
    loads[7].wait()
    mixer[...] = packed_mixer(mix_v[...])
    unmixer[...] = packed_mixer(unmix_v[...])

    pltpu.make_async_copy(shift.at[pl.ds(0, NT - 1)], shift.at[pl.ds(0, NT - 1)], shift_recv).wait()
    shifts = jnp.concatenate([shift[t, 0:1, :] for t in range(NT)], axis=0)
    for chunk in range(2):
        center = shifts + mu[mine] + tail[chunk : chunk + 1, :]

        def step(s, last, chunk=chunk, center=center):
            last = 1.0 / (center - last)
            ratio[chunk, s] = last
            return last

        lax.fori_loop(0, ROWS, step, jnp.zeros((NT, N), F32), unroll=4)

    lower = lax.broadcasted_iota(jnp.int32, (NT, N), 1) < HALF

    def mixed(matrix, first, second):
        pair = [jnp.concatenate([field, pltpu.roll(field, HALF, 1)], axis=0) for field in (first, second)]
        high, low = split(jnp.concatenate(pair, axis=1))
        both = dot(matrix, jnp.concatenate([high, low, high], axis=0))
        return [jnp.where(lower, both[:NT, k : k + N], both[NT:, k : k + N]) for k in (0, N)]

    def place(s):
        return s + h * (ROWS - 1 - 2 * s)

    def swap(chunk):
        return pltpu.make_async_remote_copy(
            swap_out.at[chunk], swap_in.at[chunk], swap_send.at[chunk], swap_recv.at[chunk],
            device_id=other, device_id_type=MESH,
        )

    def towards(chunk):
        with jax.named_scope("wait_got"):
            arrived(0, chunk, got)
        matrix = unmixer[...]

        def unmix(k, _):
            pair = (2 * k, 2 * k + 1)
            mixes = mixed(matrix, *(got[chunk, pl.ds(place(s), NT, stride=ROWS), :] for s in pair))
            for s, field in zip(pair, mixes):
                work[chunk, s] = field
            return _

        with jax.named_scope("unmix"):
            lax.fori_loop(0, ROWS // 2, unmix, 0, unroll=8)

        def step(s, last):
            last = (work[chunk, s] + last) * ratio[chunk, s]
            work[chunk, s] = last
            return last

        with jax.named_scope("eliminate"):
            swap_out[chunk] = lax.fori_loop(0, ROWS, step, jnp.zeros((NT, N), F32), unroll=8)
        swap(chunk).start()

    def away(chunk):
        with jax.named_scope("wait_swap"):
            swap(chunk).wait()
        end = ratio[chunk, ROWS - 1]
        edge = (swap_out[chunk] + end * swap_in[chunk]) / (1.0 - end * end)
        work[chunk, ROWS - 1] = edge

        def step(k, last):
            s = ROWS - 2 - k
            last = work[chunk, s] + ratio[chunk, s] * last
            work[chunk, s] = last
            return last

        with jax.named_scope("back"):
            lax.fori_loop(0, ROWS - 1, step, edge, unroll=7)
        matrix = mixer[...]

        def mix(k, _):
            pair = (2 * k, 2 * k + 1)
            for s, field in zip(pair, mixed(matrix, *(work[chunk, s] for s in pair))):
                sent_back[chunk, pl.ds(place(s), NT, stride=ROWS), :] = field
            return _

        with jax.named_scope("mix"):
            lax.fori_loop(0, ROWS // 2, mix, 0, unroll=8)
        got_back[chunk, rows(mine), :] = sent_back[chunk, rows(mine), :]

    towards(0)
    issue(0, 1, sent, got, LATE)
    away(0)
    issue(1, 0, sent_back, got_back, EARLY_BACK)
    towards(1)
    issue(1, 0, sent_back, got_back, LATE_BACK)
    away(1)
    issue(1, 1, sent_back, got_back, ORDER)

    def from_rows(chunk, i):
        pair = [got_back[chunk, pl.ds(i + k, N, stride=LOCAL), :] for k in range(2)]
        high, low = split(jnp.concatenate(pair, axis=1))
        field = dot(sine[...], jnp.concatenate([high, low, high], axis=0))
        high, low = split(field)
        for k in range(2):
            last_rows[0, i + k, :, pl.ds(chunk * N, N)] = high[:, k * N : (k + 1) * N]
            last_rows[1, i + k, :, pl.ds(chunk * N, N)] = low[:, k * N : (k + 1) * N]

    def from_columns(i):
        high, low = last_rows[0, i], last_rows[1, i]
        field = dot(jnp.concatenate([high, low, high], axis=1), back[...])
        out[0, i] = field[:, :N]
        out[1, i] = field[:, N:]

    with jax.named_scope("wait_back0"):
        arrived(1, 0, got_back)
    with jax.named_scope("last0"):
        for i in range(0, LOCAL, 2):
            from_rows(0, i)
    with jax.named_scope("wait_back1"):
        arrived(1, 1, got_back)
    with jax.named_scope("last1"):
        for i in range(0, LOCAL, 2):
            from_rows(1, i)
            if i >= 4:
                from_columns(i - 4)
                from_columns(i - 3)
        for i in range(LOCAL - 4, LOCAL):
            from_columns(i)

    for chunk in range(2):
        left(0, chunk, sent)
        left(1, chunk, sent_back)
    pltpu.make_async_copy(shift.at[pl.ds(0, NT - 1)], shift.at[pl.ds(0, NT - 1)], shift_send).wait()


def body(forcing, exponents, mixing, unmixing):
    into, back, stacked, tail, mu = constants()
    whole = pl.BlockSpec(memory_space=pltpu.HBM)
    dma = pltpu.SemaphoreType.DMA
    packed = (2, SLOTS * LOCAL, N)
    arrays = (forcing, exponents, mixing, unmixing, into, back, stacked, tail, mu)
    return pl.pallas_call(
        kernel,
        out_shape=jax.ShapeDtypeStruct(forcing.shape, F32),
        in_specs=[whole] * len(arrays),
        out_specs=pl.BlockSpec(memory_space=pltpu.VMEM),
        scratch_shapes=[
            pltpu.SMEM(exponents.shape, jnp.int32),
            pltpu.SMEM(mu.shape, F32),
            pltpu.VMEM(forcing.shape, F32),
            pltpu.VMEM((2, LOCAL, N, 2 * N), BF16),
            pltpu.VMEM(into.shape, BF16),
            pltpu.VMEM(back.shape, BF16),
            pltpu.VMEM(stacked.shape, BF16),
            pltpu.VMEM(tail.shape, F32),
            pltpu.VMEM((STEPS, STEPS), F32),
            pltpu.VMEM((STEPS, STEPS), F32),
            pltpu.VMEM((STEPS, 3 * STEPS), BF16),
            pltpu.VMEM((STEPS, 3 * STEPS), BF16),
            pltpu.VMEM(packed, F32),
            pltpu.VMEM(packed, F32),
            pltpu.VMEM((2, ROWS, NT, N), F32),
            pltpu.VMEM((2, ROWS, NT, N), F32),
            pltpu.VMEM((NT, 8, N), F32),
            pltpu.VMEM((2, NT, N), F32),
            pltpu.VMEM((2, NT, N), F32),
            pltpu.VMEM(packed, F32),
            pltpu.VMEM(packed, F32),
            pltpu.VMEM((2, LOCAL, N, 2 * N), BF16),
            dma((4,)),
            dma((8,)),
            dma((2, 2)),
            dma((2, 2)),
            dma((2,)),
            dma((2,)),
            dma,
            dma,
        ],
        compiler_params=pltpu.CompilerParams(
            collective_id=0, has_side_effects=True, vmem_limit_bytes=48 * 1024 * 1024
        ),
        name="heat",
    )(*(pltpu.with_memory_space_constraint(jnp.asarray(a), pltpu.HBM) for a in arrays))


def solution(mesh):
    placed = (P("tm", "space", None, None), P("tm"), P(), P())
    return jax.shard_map(
        body, mesh=mesh, in_specs=placed, out_specs=P("tm", "space", None, None), check_vma=False
    )
```

```python
import itertools

import jax
import jax.numpy as jnp
import numpy as np
from jax import lax
from jax.experimental import pallas as pl
from jax.experimental.pallas import tpu as pltpu
from jax.sharding import PartitionSpec as P

MESH = pl.DeviceIdType.MESH
F32, BF16 = jnp.float32, jnp.bfloat16
N, STEPS = 128, 64
NY, NZ, NC, NH, NX = 4, 4, 2, 2, 4
NT = NY * NZ * NC
LOCAL = N // (NH * NX)
ROWS = LOCAL * NX
HALF = N // 2
SLOTS = NT * NX
ORDER = (2, 1, 3, 0)
EARLY, LATE = ORDER[:1], ORDER[1:]
EARLY_BACK, LATE_BACK = ORDER[:1], ORDER[1:]
LAST = ORDER


def two_parts(x):
    x = np.asarray(x, np.float32)
    high = x.astype(jnp.bfloat16)
    low = (x - high.astype(np.float32)).astype(jnp.bfloat16)
    return high, low


def constants():
    order = np.arange(1, N + 1, dtype=np.float64)
    sine = np.sqrt(2.0 / (N + 1)) * np.sin(np.pi / (N + 1) * order[:, None] * order[None, :])
    mu = 2.0 - 2.0 * np.cos(np.pi * order / (N + 1))
    both = np.zeros((2, N, 2, 2, HALF))
    for step in range(2):
        both[step, :, :, step, :] = sine.reshape(N, 2, HALF)
    both = both.reshape(2 * N, 2 * N)
    high, low = two_parts(both)
    into = np.concatenate([high, high, low], axis=0)
    high, low = two_parts(both.T)
    back = np.stack([np.concatenate([a[k * N : (k + 1) * N] for a in (high, high, low)], axis=0) for k in range(2)])
    high, low = two_parts(sine)
    stacked = np.concatenate([high, high, low], axis=1)
    tail = np.zeros((8, N))
    for chunk in range(2):
        tail[chunk] = np.tile(mu[chunk * HALF : (chunk + 1) * HALF] + 2.0, 2)
    return into, back, stacked, tail.astype(np.float32), mu.astype(np.float32)


def split(x):
    high = x.astype(BF16)
    low = (x - high.astype(F32)).astype(BF16)
    return high, low


def dot(a, b):
    return jnp.dot(a, b, preferred_element_type=F32)


def packed_mixer(matrix):
    row = lax.broadcasted_iota(jnp.int32, (NT, STEPS), 0)
    col = lax.broadcasted_iota(jnp.int32, (NT, STEPS), 1)
    even = (col == 2 * row).astype(BF16)
    odd = (col == 2 * row + 1).astype(BF16)
    row = lax.broadcasted_iota(jnp.int32, (STEPS, STEPS), 0)
    col = lax.broadcasted_iota(jnp.int32, (STEPS, STEPS), 1)
    pos = 2 * (col - jnp.where(col >= NT, NT, 0))
    upper = jnp.where(col >= NT, 1, 0)
    even_first = (row == pos + upper).astype(BF16)
    odd_first = (row == pos + 1 - upper).astype(BF16)

    def arranged(part):
        top = dot(dot(even, part).astype(BF16), even_first)
        bottom = dot(dot(odd, part).astype(BF16), odd_first)
        return jnp.concatenate([top, bottom], axis=0).astype(BF16)

    high, low = split(matrix)
    high, low = arranged(high), arranged(low)
    return jnp.concatenate([high, high, low], axis=1)


def kernel(
    forcing, exponents_c, mixing, unmixing, into_c, back_c, sine_c, tail_c, mu_c,
    out,
    exponents, mu, x, first_rows, into, back, sine, tail, mix_v, unmix_v, mixer, unmixer,
    sent, got, work, ratio, shift, swap_out, swap_in, sent_back, got_back, last_rows,
    in_sem, const_sem, send_sem, recv_sem, swap_send, swap_recv, shift_send, shift_recv,
):
    tm, space = lax.axis_index("tm"), lax.axis_index("space")
    y, z, c = tm // (NZ * NC), (tm // NC) % NZ, tm % NC
    h, sx = space // NX, space % NX
    mine = tm * NX + sx
    zs = [z, z + 1 - 2 * (z % 2), (z + 2) % NZ, NZ - 1 - z]
    xs = [(sx + d) % NX for d in range(NX)]
    ys = [(y + d) % NY for d in range(NY)]
    cs = [(c + d) % NC for d in range(NC)]

    quarter = LOCAL // 4
    fields = [
        pltpu.make_async_copy(
            forcing.at[:, pl.ds(b * quarter, quarter)], x.at[:, pl.ds(b * quarter, quarter)], in_sem.at[b]
        )
        for b in range(4)
    ]
    pairs = (
        (into_c, into), (sine_c, sine), (exponents_c, exponents), (mu_c, mu), (tail_c, tail),
        (mixing, mix_v), (unmixing, unmix_v), (back_c, back),
    )
    loads = [pltpu.make_async_copy(a, b, const_sem.at[k]) for k, (a, b) in enumerate(pairs)]
    for load in (loads[0], *fields, *loads[1:]):
        load.start()

    barrier = pltpu.get_barrier_semaphore()
    other = (tm, (1 - h) * NX + sx)

    pl.semaphore_signal(barrier, inc=1, device_id=other, device_id_type=MESH)

    with jax.named_scope("greet"):
        steps = itertools.product(range(NX), range(NY), range(NZ), range(NC))
        farthest_first = sorted(steps, key=lambda d: -min(d[0], NX - d[0]) - min(d[1], NY - d[1]) - 2 * (d[2] > 0))
        for dx, dy, dz, dc in farthest_first[:-2] + [(0, 0, 0, 1)]:
            t = ys[dy] * (NZ * NC) + zs[dz] * NC + cs[dc]
            pl.semaphore_signal(barrier, inc=1, device_id=(t, h * NX + xs[dx]), device_id_type=MESH)

    with jax.named_scope("load"):
        loads[0].wait()
        fields[0].wait()

    def into_columns(i):
        high, low = split(jnp.concatenate([x[0, i], x[1, i]], axis=1))
        field = dot(jnp.concatenate([high, low, high], axis=1), into[...])
        high, low = split(field)
        first_rows[0, i] = high
        first_rows[1, i] = low

    def into_rows(chunk, i):
        columns = pl.ds(chunk * N, N)
        high, low = (
            jnp.concatenate([first_rows[k, i, :, columns], first_rows[k, i + 1, :, columns]], axis=1) for k in range(2)
        )
        field = dot(sine[...], jnp.concatenate([high, low, high], axis=0))
        sent[chunk, pl.ds(i, N, stride=LOCAL), :] = field[:, :N]
        sent[chunk, pl.ds(i + 1, N, stride=LOCAL), :] = field[:, N:]

    def rows(slot, part=0, parts=1):
        length = LOCAL // parts
        return pl.ds(pl.multiple_of(slot * LOCAL + part * length, length), length)

    def issue(stage, chunk, source, target, groups, *part, arrival=0):
        def start(t, px):
            pltpu.make_async_remote_copy(
                source.at[chunk, rows(t * NX + px, *part)],
                target.at[chunk, rows(mine, *part)],
                send_sem.at[stage, chunk],
                recv_sem.at[stage, chunk + arrival],
                device_id=(t, h * NX + px),
                device_id_type=MESH,
            ).start()

        for dz in groups:
            for dc in range(NC):
                tc = zs[dz] * NC + (c + dc) % NC

                @pl.loop(0 if dz or dc else 1, NY)
                def _(dy, tc=tc):
                    t = ((y + dy) % NY) * (NZ * NC) + tc
                    for dx in range(NX):
                        start(t, xs[dx])

                if not (dz or dc):
                    for dx in range(1, NX):
                        start(tm, xs[dx])

    loads[2].wait()
    loads[3].wait()
    lane = lax.broadcasted_iota(jnp.int32, (8, N), 1)
    exponent = jnp.where(lane < HALF, exponents[0].astype(F32), exponents[1].astype(F32))
    shift[tm] = jnp.exp2(exponent * 0.25)

    def shift_copy(t):
        return pltpu.make_async_remote_copy(
            shift.at[tm], shift.at[tm], shift_send, shift_recv, device_id=(t, space), device_id_type=MESH
        )

    def issue_shifts():
        for dz in ORDER:

            @pl.loop(0 if dz else 1, NY * NC)
            def _(s, dz=dz):
                t = ((y + s % NY) % NY) * (NZ * NC) + zs[dz] * NC + (c + s // NY) % NC
                shift_copy(t).start()

    for half in range(2):
        with jax.named_scope(f"first{half}"):
            for i in range(half * LOCAL // 2, (half + 1) * LOCAL // 2):
                if i and i % quarter == 0:
                    fields[i // quarter].wait()
                into_columns(i)
            if not half:
                loads[1].wait()
            for i in range(half * LOCAL // 2, (half + 1) * LOCAL // 2, 2):
                into_rows(0, i)
        if not half:
            with jax.named_scope("barrier"):
                pl.semaphore_wait(barrier, SLOTS)
            issue_shifts()
        issue(0, 0, sent, got, ORDER[:1], half, 2)

    def arrived(stage, chunk, target, part=0, parts=1):
        all_others = target.at[chunk, pl.ds(0, (SLOTS - 1) * LOCAL // parts)]
        pltpu.make_async_copy(all_others, all_others, recv_sem.at[stage, chunk + part]).wait()

    def left(stage, chunk, source):
        all_others = source.at[chunk, pl.ds(0, (SLOTS - 1) * LOCAL)]
        pltpu.make_async_copy(all_others, all_others, send_sem.at[stage, chunk]).wait()

    with jax.named_scope("issue0"):
        issue(0, 0, sent, got, ORDER[1:])
    with jax.named_scope("first2"):
        for i in range(0, LOCAL, 2):
            into_rows(1, i)
    issue(0, 1, sent, got, EARLY)
    for chunk in range(2):
        got[chunk, rows(mine), :] = sent[chunk, rows(mine), :]

    loads[4].wait()
    loads[5].wait()
    loads[6].wait()
    loads[7].wait()
    mixer[...] = packed_mixer(mix_v[...])
    unmixer[...] = packed_mixer(unmix_v[...])

    pltpu.make_async_copy(shift.at[pl.ds(0, NT - 1)], shift.at[pl.ds(0, NT - 1)], shift_recv).wait()
    shifts = jnp.concatenate([shift[t, 0:1, :] for t in range(NT)], axis=0)
    for chunk in range(2):
        center = shifts + mu[mine] + tail[chunk : chunk + 1, :]

        def step(s, last, chunk=chunk, center=center):
            last = 1.0 / (center - last)
            ratio[chunk, s] = last
            return last

        lax.fori_loop(0, ROWS, step, jnp.zeros((NT, N), F32), unroll=4)

    lower = lax.broadcasted_iota(jnp.int32, (NT, N), 1) < HALF

    def mixed(matrix, first, second):
        pair = [jnp.concatenate([field, pltpu.roll(field, HALF, 1)], axis=0) for field in (first, second)]
        high, low = split(jnp.concatenate(pair, axis=1))
        both = dot(matrix, jnp.concatenate([high, low, high], axis=0))
        return [jnp.where(lower, both[:NT, k : k + N], both[NT:, k : k + N]) for k in (0, N)]

    def place(s):
        return s + h * (ROWS - 1 - 2 * s)

    def swap(chunk):
        return pltpu.make_async_remote_copy(
            swap_out.at[chunk], swap_in.at[chunk], swap_send.at[chunk], swap_recv.at[chunk],
            device_id=other, device_id_type=MESH,
        )

    def towards(chunk):
        with jax.named_scope("wait_got"):
            arrived(0, chunk, got)
        matrix = unmixer[...]

        def unmix(k, _):
            pair = (2 * k, 2 * k + 1)
            mixes = mixed(matrix, *(got[chunk, pl.ds(place(s), NT, stride=ROWS), :] for s in pair))
            for s, field in zip(pair, mixes):
                work[chunk, s] = field
            return _

        with jax.named_scope("unmix"):
            lax.fori_loop(0, ROWS // 2, unmix, 0, unroll=8)

        def step(s, last):
            last = (work[chunk, s] + last) * ratio[chunk, s]
            work[chunk, s] = last
            return last

        with jax.named_scope("eliminate"):
            swap_out[chunk] = lax.fori_loop(0, ROWS, step, jnp.zeros((NT, N), F32), unroll=8)
        swap(chunk).start()

    def away(chunk, groups):
        with jax.named_scope("wait_swap"):
            swap(chunk).wait()
        end = ratio[chunk, ROWS - 1]
        edge = (swap_out[chunk] + end * swap_in[chunk]) / (1.0 - end * end)
        work[chunk, ROWS - 1] = edge

        def step(k, last):
            s = ROWS - 2 - k
            last = work[chunk, s] + ratio[chunk, s] * last
            work[chunk, s] = last
            return last

        with jax.named_scope("back"):
            lax.fori_loop(0, ROWS - 1, step, edge, unroll=7)
        matrix = mixer[...]

        for part in range(2):

            def mix(k, _, part=part):
                i = (k // 4) * LOCAL + part * (LOCAL // 2) + 2 * (k % 4)
                pair = (i, i + 1)
                for i, field in zip(pair, mixed(matrix, *(work[chunk, place(i)] for i in pair))):
                    sent_back[chunk, pl.ds(i, NT, stride=ROWS), :] = field
                return _

            with jax.named_scope("mix"):
                lax.fori_loop(0, ROWS // 4, mix, 0, unroll=8)
            issue(1, chunk, sent_back, got_back, groups, part, 2, arrival=part * chunk)
        got_back[chunk, rows(mine), :] = sent_back[chunk, rows(mine), :]

    towards(0)
    issue(0, 1, sent, got, LATE)
    away(0, EARLY_BACK)
    towards(1)
    issue(1, 0, sent_back, got_back, LATE_BACK)
    away(1, LAST)

    def from_rows(chunk, i):
        pair = [got_back[chunk, pl.ds(i + k, N, stride=LOCAL), :] for k in range(2)]
        high, low = split(jnp.concatenate(pair, axis=1))
        field = dot(sine[...], jnp.concatenate([high, low, high], axis=0))
        high, low = split(field)
        for k in range(2):
            last_rows[0, i + k, :, pl.ds(chunk * N, N)] = high[:, k * N : (k + 1) * N]
            last_rows[1, i + k, :, pl.ds(chunk * N, N)] = low[:, k * N : (k + 1) * N]

    def from_columns(chunk, i):
        columns = pl.ds(chunk * N, N)
        high, low = last_rows[0, i, :, columns], last_rows[1, i, :, columns]
        field = dot(jnp.concatenate([high, low, high], axis=1), back[chunk])
        for k in range(2):
            part = field[:, k * N : (k + 1) * N]
            out[k, i] = out[k, i] + part if chunk else part

    with jax.named_scope("wait_back0"):
        arrived(1, 0, got_back)
    with jax.named_scope("last0"):
        for i in range(0, LOCAL, 2):
            from_rows(0, i)
        for i in range(LOCAL):
            from_columns(0, i)
    for part in range(2):
        with jax.named_scope(f"wait_back1{part}"):
            arrived(1, 1, got_back, part, 2)
        with jax.named_scope(f"last1{part}"):
            start, end = part * LOCAL // 2, (part + 1) * LOCAL // 2
            for i in range(start, end, 2):
                from_rows(1, i)
                if i >= start + 4:
                    from_columns(1, i - 4)
                    from_columns(1, i - 3)
            for i in range(end - 4, end):
                from_columns(1, i)

    for chunk in range(2):
        left(0, chunk, sent)
        left(1, chunk, sent_back)
    pltpu.make_async_copy(shift.at[pl.ds(0, NT - 1)], shift.at[pl.ds(0, NT - 1)], shift_send).wait()


def body(forcing, exponents, mixing, unmixing):
    into, back, stacked, tail, mu = constants()
    whole = pl.BlockSpec(memory_space=pltpu.HBM)
    dma = pltpu.SemaphoreType.DMA
    packed = (2, SLOTS * LOCAL, N)
    arrays = (forcing, exponents, mixing, unmixing, into, back, stacked, tail, mu)
    return pl.pallas_call(
        kernel,
        out_shape=jax.ShapeDtypeStruct(forcing.shape, F32),
        in_specs=[whole] * len(arrays),
        out_specs=pl.BlockSpec(memory_space=pltpu.VMEM),
        scratch_shapes=[
            pltpu.SMEM(exponents.shape, jnp.int32),
            pltpu.SMEM(mu.shape, F32),
            pltpu.VMEM(forcing.shape, F32),
            pltpu.VMEM((2, LOCAL, N, 2 * N), BF16),
            pltpu.VMEM(into.shape, BF16),
            pltpu.VMEM(back.shape, BF16),
            pltpu.VMEM(stacked.shape, BF16),
            pltpu.VMEM(tail.shape, F32),
            pltpu.VMEM((STEPS, STEPS), F32),
            pltpu.VMEM((STEPS, STEPS), F32),
            pltpu.VMEM((STEPS, 3 * STEPS), BF16),
            pltpu.VMEM((STEPS, 3 * STEPS), BF16),
            pltpu.VMEM(packed, F32),
            pltpu.VMEM(packed, F32),
            pltpu.VMEM((2, ROWS, NT, N), F32),
            pltpu.VMEM((2, ROWS, NT, N), F32),
            pltpu.VMEM((NT, 8, N), F32),
            pltpu.VMEM((2, NT, N), F32),
            pltpu.VMEM((2, NT, N), F32),
            pltpu.VMEM(packed, F32),
            pltpu.VMEM(packed, F32),
            pltpu.VMEM((2, LOCAL, N, 2 * N), BF16),
            dma((4,)),
            dma((8,)),
            dma((2, 2)),
            dma((2, 3)),
            dma((2,)),
            dma((2,)),
            dma,
            dma,
        ],
        compiler_params=pltpu.CompilerParams(
            collective_id=0, has_side_effects=True, vmem_limit_bytes=48 * 1024 * 1024
        ),
        name="heat",
    )(*(pltpu.with_memory_space_constraint(jnp.asarray(a), pltpu.HBM) for a in arrays))


def solution(mesh):
    placed = (P("tm", "space", None, None), P("tm"), P(), P())
    return jax.shard_map(
        body, mesh=mesh, in_specs=placed, out_specs=P("tm", "space", None, None), check_vma=False
    )
```

```python
import itertools

import jax
import jax.numpy as jnp
import numpy as np
from jax import lax
from jax.experimental import pallas as pl
from jax.experimental.pallas import tpu as pltpu
from jax.sharding import PartitionSpec as P

MESH = pl.DeviceIdType.MESH
F32, BF16 = jnp.float32, jnp.bfloat16
N, STEPS = 128, 64
NY, NZ, NC, NH, NX = 4, 4, 2, 2, 4
NT = NY * NZ * NC
LOCAL = N // (NH * NX)
ROWS = LOCAL * NX
HALF = N // 2
SLOTS = NT * NX
ORDER = (2, 1, 3, 0)
EARLY, LATE = ORDER[:1], ORDER[1:]
EARLY_BACK, LATE_BACK = ORDER[:1], ORDER[1:]
LAST = ORDER


def two_parts(x):
    x = np.asarray(x, np.float32)
    high = x.astype(jnp.bfloat16)
    low = (x - high.astype(np.float32)).astype(jnp.bfloat16)
    return high, low


def constants():
    order = np.arange(1, N + 1, dtype=np.float64)
    sine = np.sqrt(2.0 / (N + 1)) * np.sin(np.pi / (N + 1) * order[:, None] * order[None, :])
    mu = 2.0 - 2.0 * np.cos(np.pi * order / (N + 1))
    both = np.zeros((2, N, 2, 2, HALF))
    for step in range(2):
        both[step, :, :, step, :] = sine.reshape(N, 2, HALF)
    both = both.reshape(2 * N, 2 * N)
    high, low = two_parts(both)
    into = np.concatenate([high, high, low], axis=0)
    high, low = two_parts(both.T)
    back = np.stack([np.concatenate([a[k * N : (k + 1) * N] for a in (high, high, low)], axis=0) for k in range(2)])
    high, low = two_parts(sine)
    stacked = np.concatenate([high, high, low], axis=1)
    tail = np.zeros((8, N))
    for chunk in range(2):
        tail[chunk] = np.tile(mu[chunk * HALF : (chunk + 1) * HALF] + 2.0, 2)
    return into, back, stacked, tail.astype(np.float32), mu.astype(np.float32)


def split(x):
    high = x.astype(BF16)
    low = (x - high.astype(F32)).astype(BF16)
    return high, low


def dot(a, b):
    return jnp.dot(a, b, preferred_element_type=F32)


def packed_mixer(matrix):
    row = lax.broadcasted_iota(jnp.int32, (NT, STEPS), 0)
    col = lax.broadcasted_iota(jnp.int32, (NT, STEPS), 1)
    even = (col == 2 * row).astype(BF16)
    odd = (col == 2 * row + 1).astype(BF16)
    row = lax.broadcasted_iota(jnp.int32, (STEPS, STEPS), 0)
    col = lax.broadcasted_iota(jnp.int32, (STEPS, STEPS), 1)
    pos = 2 * (col - jnp.where(col >= NT, NT, 0))
    upper = jnp.where(col >= NT, 1, 0)
    even_first = (row == pos + upper).astype(BF16)
    odd_first = (row == pos + 1 - upper).astype(BF16)

    def arranged(part):
        top = dot(dot(even, part).astype(BF16), even_first)
        bottom = dot(dot(odd, part).astype(BF16), odd_first)
        return jnp.concatenate([top, bottom], axis=0).astype(BF16)

    high, low = split(matrix)
    high, low = arranged(high), arranged(low)
    return jnp.concatenate([high, high, low], axis=1)


def kernel(
    forcing, exponents_c, mixing, unmixing, into_c, back_c, sine_c, tail_c, mu_c,
    out,
    exponents, mu, x, first_rows, into, back, sine, tail, mix_v, unmix_v, mixer, unmixer,
    sent, got, work, ratio, shift, swap_out, swap_in, sent_back, got_back, last_rows,
    in_sem, const_sem, send_sem, recv_sem, swap_send, swap_recv, shift_send, shift_recv,
):
    tm, space = lax.axis_index("tm"), lax.axis_index("space")
    y, z, c = tm // (NZ * NC), (tm // NC) % NZ, tm % NC
    h, sx = space // NX, space % NX
    mine = tm * NX + sx
    zs = [z, z + 1 - 2 * (z % 2), (z + 2) % NZ, NZ - 1 - z]
    xs = [(sx + d) % NX for d in range(NX)]
    ys = [(y + d) % NY for d in range(NY)]
    cs = [(c + d) % NC for d in range(NC)]

    quarter = LOCAL // 4
    fields = [
        pltpu.make_async_copy(
            forcing.at[:, pl.ds(b * quarter, quarter)], x.at[:, pl.ds(b * quarter, quarter)], in_sem.at[b]
        )
        for b in range(4)
    ]
    pairs = (
        (into_c, into), (sine_c, sine), (exponents_c, exponents), (mu_c, mu), (tail_c, tail),
        (mixing, mix_v), (unmixing, unmix_v), (back_c, back),
    )
    loads = [pltpu.make_async_copy(a, b, const_sem.at[k]) for k, (a, b) in enumerate(pairs)]
    for load in (loads[0], *fields, *loads[1:]):
        load.start()

    barrier = pltpu.get_barrier_semaphore()
    other = (tm, (1 - h) * NX + sx)

    pl.semaphore_signal(barrier, inc=1, device_id=other, device_id_type=MESH)

    with jax.named_scope("greet"):
        steps = itertools.product(range(NX), range(NY), range(NZ), range(NC))
        farthest_first = sorted(steps, key=lambda d: -min(d[0], NX - d[0]) - min(d[1], NY - d[1]) - 2 * (d[2] > 0))
        for dx, dy, dz, dc in farthest_first[:-2] + [(0, 0, 0, 1)]:
            t = ys[dy] * (NZ * NC) + zs[dz] * NC + cs[dc]
            pl.semaphore_signal(barrier, inc=1, device_id=(t, h * NX + xs[dx]), device_id_type=MESH)

    with jax.named_scope("load"):
        loads[0].wait()
        fields[0].wait()

    def into_columns(i):
        high, low = split(jnp.concatenate([x[0, i], x[1, i]], axis=1))
        field = dot(jnp.concatenate([high, low, high], axis=1), into[...])
        high, low = split(field)
        first_rows[0, i] = high
        first_rows[1, i] = low

    def into_rows(chunk, i):
        columns = pl.ds(chunk * N, N)
        high, low = (
            jnp.concatenate([first_rows[k, i, :, columns], first_rows[k, i + 1, :, columns]], axis=1) for k in range(2)
        )
        field = dot(sine[...], jnp.concatenate([high, low, high], axis=0))
        sent[chunk, pl.ds(i, N, stride=LOCAL), :] = field[:, :N]
        sent[chunk, pl.ds(i + 1, N, stride=LOCAL), :] = field[:, N:]

    def rows(slot, part=0, parts=1):
        length = LOCAL // parts
        return pl.ds(pl.multiple_of(slot * LOCAL + part * length, length), length)

    def issue(stage, chunk, source, target, groups, *part, arrival=0):
        def start(t, px):
            pltpu.make_async_remote_copy(
                source.at[chunk, rows(t * NX + px, *part)],
                target.at[chunk, rows(mine, *part)],
                send_sem.at[stage, chunk],
                recv_sem.at[stage, chunk + arrival],
                device_id=(t, h * NX + px),
                device_id_type=MESH,
            ).start()

        for dz in groups:
            for dc in range(NC):
                tc = zs[dz] * NC + (c + dc) % NC

                @pl.loop(0 if dz or dc else 1, NY)
                def _(dy, tc=tc):
                    t = ((y + dy) % NY) * (NZ * NC) + tc
                    for dx in range(NX):
                        start(t, xs[dx])

                if not (dz or dc):
                    for dx in range(1, NX):
                        start(tm, xs[dx])

    loads[2].wait()
    loads[3].wait()
    lane = lax.broadcasted_iota(jnp.int32, (1, N), 1)
    exponent = jnp.where(lane < HALF, exponents[0].astype(F32), exponents[1].astype(F32))
    shift[tm] = jnp.exp2(exponent * 0.25)

    def shift_copy(t):
        return pltpu.make_async_remote_copy(
            shift.at[tm], shift.at[tm], shift_send, shift_recv, device_id=(t, space), device_id_type=MESH
        )

    def issue_shifts():
        for dz in ORDER:

            @pl.loop(0 if dz else 1, NY * NC)
            def _(s, dz=dz):
                t = ((y + s % NY) % NY) * (NZ * NC) + zs[dz] * NC + (c + s // NY) % NC
                shift_copy(t).start()

    for half in range(2):
        with jax.named_scope(f"first{half}"):
            for i in range(half * LOCAL // 2, (half + 1) * LOCAL // 2):
                if i and i % quarter == 0:
                    fields[i // quarter].wait()
                into_columns(i)
            if not half:
                loads[1].wait()
            for i in range(half * LOCAL // 2, (half + 1) * LOCAL // 2, 2):
                into_rows(0, i)
        if not half:
            with jax.named_scope("barrier"):
                pl.semaphore_wait(barrier, SLOTS)
            issue_shifts()
        issue(0, 0, sent, got, ORDER[:1], half, 2)

    def arrived(stage, chunk, target, part=0, parts=1):
        all_others = target.at[chunk, pl.ds(0, (SLOTS - 1) * LOCAL // parts)]
        pltpu.make_async_copy(all_others, all_others, recv_sem.at[stage, chunk + part]).wait()

    def left(stage, chunk, source):
        all_others = source.at[chunk, pl.ds(0, (SLOTS - 1) * LOCAL)]
        pltpu.make_async_copy(all_others, all_others, send_sem.at[stage, chunk]).wait()

    with jax.named_scope("issue0"):
        issue(0, 0, sent, got, ORDER[1:])
    with jax.named_scope("first2"):
        for i in range(0, LOCAL, 2):
            into_rows(1, i)
    issue(0, 1, sent, got, EARLY)
    for chunk in range(2):
        got[chunk, rows(mine), :] = sent[chunk, rows(mine), :]

    loads[4].wait()
    loads[5].wait()
    loads[6].wait()
    loads[7].wait()
    mixer[...] = packed_mixer(mix_v[...])
    unmixer[...] = packed_mixer(unmix_v[...])

    pltpu.make_async_copy(shift.at[pl.ds(0, NT - 1)], shift.at[pl.ds(0, NT - 1)], shift_recv).wait()
    shifts = jnp.concatenate([shift[t, 0:1, :] for t in range(NT)], axis=0)
    for chunk in range(2):
        center = shifts + mu[mine] + tail[chunk : chunk + 1, :]

        def step(s, last, chunk=chunk, center=center):
            last = 1.0 / (center - last)
            ratio[chunk, s] = last
            return last

        lax.fori_loop(0, ROWS, step, jnp.zeros((NT, N), F32), unroll=4)

    lower = lax.broadcasted_iota(jnp.int32, (NT, N), 1) < HALF

    def mixed(matrix, first, second):
        pair = [jnp.concatenate([field, pltpu.roll(field, HALF, 1)], axis=0) for field in (first, second)]
        high, low = split(jnp.concatenate(pair, axis=1))
        both = dot(matrix, jnp.concatenate([high, low, high], axis=0))
        return [jnp.where(lower, both[:NT, k : k + N], both[NT:, k : k + N]) for k in (0, N)]

    def place(s):
        return s + h * (ROWS - 1 - 2 * s)

    def swap(chunk):
        return pltpu.make_async_remote_copy(
            swap_out.at[chunk], swap_in.at[chunk], swap_send.at[chunk], swap_recv.at[chunk],
            device_id=other, device_id_type=MESH,
        )

    def towards(chunk):
        with jax.named_scope("wait_got"):
            arrived(0, chunk, got)
        matrix = unmixer[...]

        def unmix(k, _):
            pair = (2 * k, 2 * k + 1)
            mixes = mixed(matrix, *(got[chunk, pl.ds(place(s), NT, stride=ROWS), :] for s in pair))
            for s, field in zip(pair, mixes):
                work[chunk, s] = field
            return _

        with jax.named_scope("unmix"):
            lax.fori_loop(0, ROWS // 2, unmix, 0, unroll=8)

        def step(s, last):
            last = (work[chunk, s] + last) * ratio[chunk, s]
            work[chunk, s] = last
            return last

        with jax.named_scope("eliminate"):
            swap_out[chunk] = lax.fori_loop(0, ROWS, step, jnp.zeros((NT, N), F32), unroll=8)
        swap(chunk).start()

    def away(chunk, groups):
        with jax.named_scope("wait_swap"):
            swap(chunk).wait()
        end = ratio[chunk, ROWS - 1]
        edge = (swap_out[chunk] + end * swap_in[chunk]) / (1.0 - end * end)
        work[chunk, ROWS - 1] = edge

        def step(k, last):
            s = ROWS - 2 - k
            last = work[chunk, s] + ratio[chunk, s] * last
            work[chunk, s] = last
            return last

        with jax.named_scope("back"):
            lax.fori_loop(0, ROWS - 1, step, edge, unroll=7)
        matrix = mixer[...]

        for part in range(2):

            def mix(k, _, part=part):
                i = (k // 4) * LOCAL + part * (LOCAL // 2) + 2 * (k % 4)
                pair = (i, i + 1)
                for i, field in zip(pair, mixed(matrix, *(work[chunk, place(i)] for i in pair))):
                    sent_back[chunk, pl.ds(i, NT, stride=ROWS), :] = field
                return _

            with jax.named_scope("mix"):
                lax.fori_loop(0, ROWS // 4, mix, 0, unroll=8)
            issue(1, chunk, sent_back, got_back, groups, part, 2, arrival=part * chunk)
        got_back[chunk, rows(mine), :] = sent_back[chunk, rows(mine), :]

    towards(0)
    issue(0, 1, sent, got, LATE)
    away(0, EARLY_BACK)
    towards(1)
    issue(1, 0, sent_back, got_back, LATE_BACK)
    away(1, LAST)

    def from_rows(chunk, i):
        pair = [got_back[chunk, pl.ds(i + k, N, stride=LOCAL), :] for k in range(2)]
        high, low = split(jnp.concatenate(pair, axis=1))
        field = dot(sine[...], jnp.concatenate([high, low, high], axis=0))
        high, low = split(field)
        for k in range(2):
            last_rows[0, i + k, :, pl.ds(chunk * N, N)] = high[:, k * N : (k + 1) * N]
            last_rows[1, i + k, :, pl.ds(chunk * N, N)] = low[:, k * N : (k + 1) * N]

    def from_columns(chunk, i):
        columns = pl.ds(chunk * N, N)
        high, low = last_rows[0, i, :, columns], last_rows[1, i, :, columns]
        field = dot(jnp.concatenate([high, low, high], axis=1), back[chunk])
        for k in range(2):
            part = field[:, k * N : (k + 1) * N]
            out[k, i] = out[k, i] + part if chunk else part

    with jax.named_scope("wait_back0"):
        arrived(1, 0, got_back)
    with jax.named_scope("last0"):
        for i in range(0, LOCAL, 2):
            from_rows(0, i)
        for i in range(LOCAL):
            from_columns(0, i)
    for part in range(2):
        with jax.named_scope(f"wait_back1{part}"):
            arrived(1, 1, got_back, part, 2)
        with jax.named_scope(f"last1{part}"):
            start, end = part * LOCAL // 2, (part + 1) * LOCAL // 2
            for i in range(start, end, 2):
                from_rows(1, i)
                if i >= start + 4:
                    from_columns(1, i - 4)
                    from_columns(1, i - 3)
            for i in range(end - 4, end):
                from_columns(1, i)

    for chunk in range(2):
        left(0, chunk, sent)
        left(1, chunk, sent_back)
    pltpu.make_async_copy(shift.at[pl.ds(0, NT - 1)], shift.at[pl.ds(0, NT - 1)], shift_send).wait()


def body(forcing, exponents, mixing, unmixing):
    into, back, stacked, tail, mu = constants()
    whole = pl.BlockSpec(memory_space=pltpu.HBM)
    dma = pltpu.SemaphoreType.DMA
    packed = (2, SLOTS * LOCAL, N)
    arrays = (forcing, exponents, mixing, unmixing, into, back, stacked, tail, mu)
    return pl.pallas_call(
        kernel,
        out_shape=jax.ShapeDtypeStruct(forcing.shape, F32),
        in_specs=[whole] * len(arrays),
        out_specs=pl.BlockSpec(memory_space=pltpu.VMEM),
        scratch_shapes=[
            pltpu.SMEM(exponents.shape, jnp.int32),
            pltpu.SMEM(mu.shape, F32),
            pltpu.VMEM(forcing.shape, F32),
            pltpu.VMEM((2, LOCAL, N, 2 * N), BF16),
            pltpu.VMEM(into.shape, BF16),
            pltpu.VMEM(back.shape, BF16),
            pltpu.VMEM(stacked.shape, BF16),
            pltpu.VMEM(tail.shape, F32),
            pltpu.VMEM((STEPS, STEPS), F32),
            pltpu.VMEM((STEPS, STEPS), F32),
            pltpu.VMEM((STEPS, 3 * STEPS), BF16),
            pltpu.VMEM((STEPS, 3 * STEPS), BF16),
            pltpu.VMEM(packed, F32),
            pltpu.VMEM(packed, F32),
            pltpu.VMEM((2, ROWS, NT, N), F32),
            pltpu.VMEM((2, ROWS, NT, N), F32),
            pltpu.VMEM((NT, 1, N), F32),
            pltpu.VMEM((2, NT, N), F32),
            pltpu.VMEM((2, NT, N), F32),
            pltpu.VMEM(packed, F32),
            pltpu.VMEM(packed, F32),
            pltpu.VMEM((2, LOCAL, N, 2 * N), BF16),
            dma((4,)),
            dma((8,)),
            dma((2, 2)),
            dma((2, 3)),
            dma((2,)),
            dma((2,)),
            dma,
            dma,
        ],
        compiler_params=pltpu.CompilerParams(
            collective_id=0, has_side_effects=True, vmem_limit_bytes=48 * 1024 * 1024
        ),
        name="heat",
    )(*(pltpu.with_memory_space_constraint(jnp.asarray(a), pltpu.HBM) for a in arrays))


def solution(mesh):
    placed = (P("tm", "space", None, None), P("tm"), P(), P())
    return jax.shard_map(
        body, mesh=mesh, in_specs=placed, out_specs=P("tm", "space", None, None), check_vma=False
    )
```

```python
import itertools

import jax
import jax.numpy as jnp
import numpy as np
from jax import lax
from jax.experimental import pallas as pl
from jax.experimental.pallas import tpu as pltpu
from jax.sharding import PartitionSpec as P

MESH = pl.DeviceIdType.MESH
F32, BF16 = jnp.float32, jnp.bfloat16
N, STEPS = 128, 64
NY, NZ, NC, NH, NX = 4, 4, 2, 2, 4
NT = NY * NZ * NC
LOCAL = N // (NH * NX)
ROWS = LOCAL * NX
HALF = N // 2
SLOTS = NT * NX
ORDER = (2, 1, 3, 0)
EARLY, LATE = ORDER[:1], ORDER[1:]
EARLY_BACK, LATE_BACK = ORDER[:1], ORDER[1:]
LAST = ORDER


def two_parts(x):
    x = np.asarray(x, np.float32)
    high = x.astype(jnp.bfloat16)
    low = (x - high.astype(np.float32)).astype(jnp.bfloat16)
    return high, low


def constants():
    order = np.arange(1, N + 1, dtype=np.float64)
    sine = np.sqrt(2.0 / (N + 1)) * np.sin(np.pi / (N + 1) * order[:, None] * order[None, :])
    mu = 2.0 - 2.0 * np.cos(np.pi * order / (N + 1))
    both = np.zeros((2, N, 2, 2, HALF))
    for step in range(2):
        both[step, :, :, step, :] = sine.reshape(N, 2, HALF)
    both = both.reshape(2 * N, 2 * N)
    high, low = two_parts(both)
    into = np.concatenate([high, high, low], axis=0)
    high, low = two_parts(both.T)
    back = np.stack([np.concatenate([a[k * N : (k + 1) * N] for a in (high, high, low)], axis=0) for k in range(2)])
    high, low = two_parts(sine)
    stacked = np.concatenate([high, high, low], axis=1)
    tail = np.zeros((8, N))
    for chunk in range(2):
        tail[chunk] = np.tile(mu[chunk * HALF : (chunk + 1) * HALF] + 2.0, 2)
    return into, back, stacked, tail.astype(np.float32), mu.astype(np.float32)


def split(x):
    high = x.astype(BF16)
    low = (x - high.astype(F32)).astype(BF16)
    return high, low


def dot(a, b):
    return jnp.dot(a, b, preferred_element_type=F32)


def packed_mixer(matrix):
    row = lax.broadcasted_iota(jnp.int32, (NT, STEPS), 0)
    col = lax.broadcasted_iota(jnp.int32, (NT, STEPS), 1)
    even = (col == 2 * row).astype(BF16)
    odd = (col == 2 * row + 1).astype(BF16)
    row = lax.broadcasted_iota(jnp.int32, (STEPS, STEPS), 0)
    col = lax.broadcasted_iota(jnp.int32, (STEPS, STEPS), 1)
    pos = 2 * (col - jnp.where(col >= NT, NT, 0))
    upper = jnp.where(col >= NT, 1, 0)
    even_first = (row == pos + upper).astype(BF16)
    odd_first = (row == pos + 1 - upper).astype(BF16)

    def arranged(part):
        top = dot(dot(even, part).astype(BF16), even_first)
        bottom = dot(dot(odd, part).astype(BF16), odd_first)
        return jnp.concatenate([top, bottom], axis=0).astype(BF16)

    high, low = split(matrix)
    high, low = arranged(high), arranged(low)
    return jnp.concatenate([high, high, low], axis=1)


def kernel(
    forcing, exponents_c, mixing, unmixing, into_c, back_c, sine_c, tail_c, mu_c,
    out,
    exponents, mu, x, first_rows, into, back, sine, tail, mix_v, unmix_v, mixer, unmixer,
    sent, got, work, ratio, shift, swap_out, swap_in, sent_back, got_back, last_rows,
    in_sem, const_sem, send_sem, recv_sem, swap_send, swap_recv, shift_send, shift_recv,
):
    tm, space = lax.axis_index("tm"), lax.axis_index("space")
    y, z, c = tm // (NZ * NC), (tm // NC) % NZ, tm % NC
    h, sx = space // NX, space % NX
    mine = tm * NX + sx
    zs = [z, z + 1 - 2 * (z % 2), (z + 2) % NZ, NZ - 1 - z]
    xs = [(sx + d) % NX for d in range(NX)]
    ys = [(y + d) % NY for d in range(NY)]
    cs = [(c + d) % NC for d in range(NC)]

    quarter = LOCAL // 4
    fields = [
        pltpu.make_async_copy(
            forcing.at[:, pl.ds(b * quarter, quarter)], x.at[:, pl.ds(b * quarter, quarter)], in_sem.at[b]
        )
        for b in range(4)
    ]
    pairs = (
        (into_c, into), (sine_c, sine), (exponents_c, exponents), (mu_c, mu), (tail_c, tail),
        (mixing, mix_v), (unmixing, unmix_v), (back_c, back),
    )
    loads = [pltpu.make_async_copy(a, b, const_sem.at[k]) for k, (a, b) in enumerate(pairs)]
    for load in (loads[0], *fields, *loads[1:]):
        load.start()

    barrier = pltpu.get_barrier_semaphore()
    other = (tm, (1 - h) * NX + sx)

    pl.semaphore_signal(barrier, inc=1, device_id=other, device_id_type=MESH)

    with jax.named_scope("greet"):
        steps = itertools.product(range(NX), range(NY), range(NZ), range(NC))
        farthest_first = sorted(steps, key=lambda d: -min(d[0], NX - d[0]) - min(d[1], NY - d[1]) - 2 * (d[2] > 0))
        for dx, dy, dz, dc in farthest_first[:-2] + [(0, 0, 0, 1)]:
            t = ys[dy] * (NZ * NC) + zs[dz] * NC + cs[dc]
            pl.semaphore_signal(barrier, inc=1, device_id=(t, h * NX + xs[dx]), device_id_type=MESH)

    with jax.named_scope("load"):
        loads[0].wait()
        fields[0].wait()

    def into_columns(i):
        high, low = split(jnp.concatenate([x[0, i], x[1, i]], axis=1))
        field = dot(jnp.concatenate([high, low, high], axis=1), into[...])
        high, low = split(field)
        first_rows[0, i] = high
        first_rows[1, i] = low

    def into_rows(chunk, i):
        columns = pl.ds(chunk * N, N)
        high, low = (
            jnp.concatenate([first_rows[k, i, :, columns], first_rows[k, i + 1, :, columns]], axis=1) for k in range(2)
        )
        field = dot(sine[...], jnp.concatenate([high, low, high], axis=0))
        sent[chunk, pl.ds(i, N, stride=LOCAL), :] = field[:, :N]
        sent[chunk, pl.ds(i + 1, N, stride=LOCAL), :] = field[:, N:]

    def rows(slot, part=0, parts=1):
        length = LOCAL // parts
        return pl.ds(pl.multiple_of(slot * LOCAL + part * length, length), length)

    def issue(stage, chunk, source, target, groups, *part, arrival=0):
        def start(t, px):
            pltpu.make_async_remote_copy(
                source.at[chunk, rows(t * NX + px, *part)],
                target.at[chunk, rows(mine, *part)],
                send_sem.at[stage, chunk],
                recv_sem.at[stage, chunk + arrival],
                device_id=(t, h * NX + px),
                device_id_type=MESH,
            ).start()

        for dz in groups:
            for dc in range(NC):
                tc = zs[dz] * NC + (c + dc) % NC

                @pl.loop(0 if dz or dc else 1, NY)
                def _(dy, tc=tc):
                    t = ((y + dy) % NY) * (NZ * NC) + tc
                    for dx in range(NX):
                        start(t, xs[dx])

                if not (dz or dc):
                    for dx in range(1, NX):
                        start(tm, xs[dx])

    loads[2].wait()
    loads[3].wait()
    lane = lax.broadcasted_iota(jnp.int32, (1, N), 1)
    exponent = jnp.where(lane < HALF, exponents[0].astype(F32), exponents[1].astype(F32))
    shift[tm] = jnp.exp2(exponent * 0.25)

    def shift_copy(t):
        return pltpu.make_async_remote_copy(
            shift.at[tm], shift.at[tm], shift_send, shift_recv, device_id=(t, space), device_id_type=MESH
        )

    def issue_shifts():
        for dz in ORDER:

            @pl.loop(0 if dz else 1, NY * NC)
            def _(s, dz=dz):
                t = ((y + s % NY) % NY) * (NZ * NC) + zs[dz] * NC + (c + s // NY) % NC
                shift_copy(t).start()

    for half in range(2):
        with jax.named_scope(f"first{half}"):
            for i in range(half * LOCAL // 2, (half + 1) * LOCAL // 2):
                if i and i % quarter == 0:
                    fields[i // quarter].wait()
                into_columns(i)
            if not half:
                loads[1].wait()
            for i in range(half * LOCAL // 2, (half + 1) * LOCAL // 2, 2):
                into_rows(0, i)
        if not half:
            with jax.named_scope("barrier"):
                pl.semaphore_wait(barrier, SLOTS)
        issue(0, 0, sent, got, ORDER[:1], half, 2)
        if not half:
            issue_shifts()

    def arrived(stage, chunk, target, part=0, parts=1):
        all_others = target.at[chunk, pl.ds(0, (SLOTS - 1) * LOCAL // parts)]
        pltpu.make_async_copy(all_others, all_others, recv_sem.at[stage, chunk + part]).wait()

    def left(stage, chunk, source):
        all_others = source.at[chunk, pl.ds(0, (SLOTS - 1) * LOCAL)]
        pltpu.make_async_copy(all_others, all_others, send_sem.at[stage, chunk]).wait()

    with jax.named_scope("issue0"):
        issue(0, 0, sent, got, ORDER[1:])
    with jax.named_scope("first2"):
        for i in range(0, LOCAL, 2):
            into_rows(1, i)
    issue(0, 1, sent, got, EARLY)
    for chunk in range(2):
        got[chunk, rows(mine), :] = sent[chunk, rows(mine), :]

    loads[4].wait()
    loads[5].wait()
    loads[6].wait()
    loads[7].wait()
    mixer[...] = packed_mixer(mix_v[...])
    unmixer[...] = packed_mixer(unmix_v[...])

    pltpu.make_async_copy(shift.at[pl.ds(0, NT - 1)], shift.at[pl.ds(0, NT - 1)], shift_recv).wait()
    shifts = jnp.concatenate([shift[t, 0:1, :] for t in range(NT)], axis=0)
    for chunk in range(2):
        center = shifts + mu[mine] + tail[chunk : chunk + 1, :]

        def step(s, last, chunk=chunk, center=center):
            last = 1.0 / (center - last)
            ratio[chunk, s] = last
            return last

        lax.fori_loop(0, ROWS, step, jnp.zeros((NT, N), F32), unroll=4)

    lower = lax.broadcasted_iota(jnp.int32, (NT, N), 1) < HALF

    def mixed(matrix, first, second):
        pair = [jnp.concatenate([field, pltpu.roll(field, HALF, 1)], axis=0) for field in (first, second)]
        high, low = split(jnp.concatenate(pair, axis=1))
        both = dot(matrix, jnp.concatenate([high, low, high], axis=0))
        return [jnp.where(lower, both[:NT, k : k + N], both[NT:, k : k + N]) for k in (0, N)]

    def place(s):
        return s + h * (ROWS - 1 - 2 * s)

    def swap(chunk):
        return pltpu.make_async_remote_copy(
            swap_out.at[chunk], swap_in.at[chunk], swap_send.at[chunk], swap_recv.at[chunk],
            device_id=other, device_id_type=MESH,
        )

    def towards(chunk):
        with jax.named_scope("wait_got"):
            arrived(0, chunk, got)
        matrix = unmixer[...]

        def unmix(k, _):
            pair = (2 * k, 2 * k + 1)
            mixes = mixed(matrix, *(got[chunk, pl.ds(place(s), NT, stride=ROWS), :] for s in pair))
            for s, field in zip(pair, mixes):
                work[chunk, s] = field
            return _

        with jax.named_scope("unmix"):
            lax.fori_loop(0, ROWS // 2, unmix, 0, unroll=8)

        def step(s, last):
            last = (work[chunk, s] + last) * ratio[chunk, s]
            work[chunk, s] = last
            return last

        with jax.named_scope("eliminate"):
            swap_out[chunk] = lax.fori_loop(0, ROWS, step, jnp.zeros((NT, N), F32), unroll=8)
        swap(chunk).start()

    def away(chunk, groups):
        with jax.named_scope("wait_swap"):
            swap(chunk).wait()
        end = ratio[chunk, ROWS - 1]
        edge = (swap_out[chunk] + end * swap_in[chunk]) / (1.0 - end * end)
        work[chunk, ROWS - 1] = edge

        def step(k, last):
            s = ROWS - 2 - k
            last = work[chunk, s] + ratio[chunk, s] * last
            work[chunk, s] = last
            return last

        with jax.named_scope("back"):
            lax.fori_loop(0, ROWS - 1, step, edge, unroll=7)
        matrix = mixer[...]

        for part in range(2):

            def mix(k, _, part=part):
                i = (k // 4) * LOCAL + part * (LOCAL // 2) + 2 * (k % 4)
                pair = (i, i + 1)
                for i, field in zip(pair, mixed(matrix, *(work[chunk, place(i)] for i in pair))):
                    sent_back[chunk, pl.ds(i, NT, stride=ROWS), :] = field
                return _

            with jax.named_scope("mix"):
                lax.fori_loop(0, ROWS // 4, mix, 0, unroll=8)
            issue(1, chunk, sent_back, got_back, groups, part, 2, arrival=part * chunk)
        got_back[chunk, rows(mine), :] = sent_back[chunk, rows(mine), :]

    towards(0)
    issue(0, 1, sent, got, LATE)
    away(0, EARLY_BACK)
    towards(1)
    issue(1, 0, sent_back, got_back, LATE_BACK)
    away(1, LAST)

    def from_rows(chunk, i):
        pair = [got_back[chunk, pl.ds(i + k, N, stride=LOCAL), :] for k in range(2)]
        high, low = split(jnp.concatenate(pair, axis=1))
        field = dot(sine[...], jnp.concatenate([high, low, high], axis=0))
        high, low = split(field)
        for k in range(2):
            last_rows[0, i + k, :, pl.ds(chunk * N, N)] = high[:, k * N : (k + 1) * N]
            last_rows[1, i + k, :, pl.ds(chunk * N, N)] = low[:, k * N : (k + 1) * N]

    def from_columns(chunk, i):
        columns = pl.ds(chunk * N, N)
        high, low = last_rows[0, i, :, columns], last_rows[1, i, :, columns]
        field = dot(jnp.concatenate([high, low, high], axis=1), back[chunk])
        for k in range(2):
            part = field[:, k * N : (k + 1) * N]
            out[k, i] = out[k, i] + part if chunk else part

    with jax.named_scope("wait_back0"):
        arrived(1, 0, got_back)
    with jax.named_scope("last0"):
        for i in range(0, LOCAL, 2):
            from_rows(0, i)
        for i in range(LOCAL):
            from_columns(0, i)
    for part in range(2):
        with jax.named_scope(f"wait_back1{part}"):
            arrived(1, 1, got_back, part, 2)
        with jax.named_scope(f"last1{part}"):
            start, end = part * LOCAL // 2, (part + 1) * LOCAL // 2
            for i in range(start, end, 2):
                from_rows(1, i)
                if i >= start + 4:
                    from_columns(1, i - 4)
                    from_columns(1, i - 3)
            for i in range(end - 4, end):
                from_columns(1, i)

    for chunk in range(2):
        left(0, chunk, sent)
        left(1, chunk, sent_back)
    pltpu.make_async_copy(shift.at[pl.ds(0, NT - 1)], shift.at[pl.ds(0, NT - 1)], shift_send).wait()


def body(forcing, exponents, mixing, unmixing):
    into, back, stacked, tail, mu = constants()
    whole = pl.BlockSpec(memory_space=pltpu.HBM)
    dma = pltpu.SemaphoreType.DMA
    packed = (2, SLOTS * LOCAL, N)
    arrays = (forcing, exponents, mixing, unmixing, into, back, stacked, tail, mu)
    return pl.pallas_call(
        kernel,
        out_shape=jax.ShapeDtypeStruct(forcing.shape, F32),
        in_specs=[whole] * len(arrays),
        out_specs=pl.BlockSpec(memory_space=pltpu.VMEM),
        scratch_shapes=[
            pltpu.SMEM(exponents.shape, jnp.int32),
            pltpu.SMEM(mu.shape, F32),
            pltpu.VMEM(forcing.shape, F32),
            pltpu.VMEM((2, LOCAL, N, 2 * N), BF16),
            pltpu.VMEM(into.shape, BF16),
            pltpu.VMEM(back.shape, BF16),
            pltpu.VMEM(stacked.shape, BF16),
            pltpu.VMEM(tail.shape, F32),
            pltpu.VMEM((STEPS, STEPS), F32),
            pltpu.VMEM((STEPS, STEPS), F32),
            pltpu.VMEM((STEPS, 3 * STEPS), BF16),
            pltpu.VMEM((STEPS, 3 * STEPS), BF16),
            pltpu.VMEM(packed, F32),
            pltpu.VMEM(packed, F32),
            pltpu.VMEM((2, ROWS, NT, N), F32),
            pltpu.VMEM((2, ROWS, NT, N), F32),
            pltpu.VMEM((NT, 1, N), F32),
            pltpu.VMEM((2, NT, N), F32),
            pltpu.VMEM((2, NT, N), F32),
            pltpu.VMEM(packed, F32),
            pltpu.VMEM(packed, F32),
            pltpu.VMEM((2, LOCAL, N, 2 * N), BF16),
            dma((4,)),
            dma((8,)),
            dma((2, 2)),
            dma((2, 3)),
            dma((2,)),
            dma((2,)),
            dma,
            dma,
        ],
        compiler_params=pltpu.CompilerParams(
            collective_id=0, has_side_effects=True, vmem_limit_bytes=48 * 1024 * 1024
        ),
        name="heat",
    )(*(pltpu.with_memory_space_constraint(jnp.asarray(a), pltpu.HBM) for a in arrays))


def solution(mesh):
    placed = (P("tm", "space", None, None), P("tm"), P(), P())
    return jax.shard_map(
        body, mesh=mesh, in_specs=placed, out_specs=P("tm", "space", None, None), check_vma=False
    )
```
